8 devices in a mesh: dp: 1 (over z), fsdp: 2 (over y), sp: 4 (over x, core).
Axes of the slice: x: 2, y: 2, z: 1, core: 2. Of those that a mesh axis runs over, the one named last changes fastest.
Arguments:
- x_in: bfloat16 [32, 512, 4096], P(('dp', 'fsdp'), 'sp')
- norm_attn: bfloat16 [4096], P('fsdp')
- w_query: bfloat16 [4096, 4096], P('fsdp')
- w_key: bfloat16 [4096, 4096], P('fsdp')
- w_value: bfloat16 [4096, 4096], P('fsdp')
- w_out: bfloat16 [4096, 4096], P('fsdp')
- norm_mlp: bfloat16 [4096], P('fsdp')
- w_gate: bfloat16 [4096, 11008], P('fsdp')
- w_up: bfloat16 [4096, 11008], P('fsdp')
- w_down: bfloat16 [11008, 4096], P('fsdp')
Outputs:
- output: bfloat16 [32, 512, 4096], P(('dp', 'fsdp'), 'sp')
All inputs are finite; a program needn't handle non-finite values.
Results may differ from the reference program's by a relative error of at most 0.0114426.
Values are sent between devices in bfloat16 or wider.
A program may use at most 1 GiB of HBM per device.

```python
import math
import jax
import jax.numpy as jnp
from jax import lax

MODEL_DIM = 4096
NUM_HEADS = 32
FFN_DIM = 11008
NUM_ROWS = 32
SEQ_SHARDS = 4
SHARD_LEN = 128
QUERY_BLOCK = 32

HEAD_DIM = MODEL_DIM // NUM_HEADS
SEQ_LEN = SEQ_SHARDS * SHARD_LEN
ANCHOR_GAP = 2 * SEQ_SHARDS
NORM_EPS = 1e-5
ROPE_THETA = 5e7
MASK_VALUE = -1e30


def dealt_order(natural):
    lead_rows = natural.shape[0]
    tail_shape = natural.shape[2:]
    token_grid = natural.reshape((lead_rows, SHARD_LEN, SEQ_SHARDS) + tail_shape)
    return jnp.swapaxes(token_grid, 1, 2).reshape((lead_rows, SEQ_LEN) + tail_shape)


def draw_tokens(rng_key):
    key_anchor, key_noise = jax.random.split(rng_key)
    anchors = jax.random.normal(key_anchor, (NUM_ROWS, SEQ_LEN // ANCHOR_GAP + 1, MODEL_DIM), jnp.float32)
    ramp_wts = (jnp.arange(ANCHOR_GAP, dtype=jnp.float32) / ANCHOR_GAP)[None, None, :, None]
    smooth = (1.0 - ramp_wts) * anchors[:, :-1, None, :] + ramp_wts * anchors[:, 1:, None, :]
    smooth = smooth.reshape(NUM_ROWS, SEQ_LEN, MODEL_DIM)
    noise_part = jax.random.normal(key_noise, (NUM_ROWS, SEQ_LEN, MODEL_DIM), jnp.float32)
    return dealt_order(smooth + 0.3 * noise_part).astype(jnp.bfloat16)


def draw_matrix(rng_key, fan_in, fan_out):
    return jax.random.normal(rng_key, (fan_in, fan_out), jnp.float32) * fan_in ** -0.5


def draw_gain(rng_key):
    return jax.random.uniform(rng_key, (MODEL_DIM,), jnp.float32, 0.5, 1.5).astype(jnp.bfloat16)


def setup_inputs(seed: int = 0, part: int = 0) -> dict:
    root_key = jax.random.key(seed)
    shared_keys = jax.random.split(jax.random.fold_in(root_key, 100003), 9)
    query_w = draw_matrix(shared_keys[1], MODEL_DIM, MODEL_DIM)
    key_w = 0.8 * query_w + 0.6 * draw_matrix(shared_keys[2], MODEL_DIM, MODEL_DIM)
    return {
        'x_in': draw_tokens(jax.random.fold_in(root_key, part)),
        'norm_attn': draw_gain(shared_keys[0]),
        'w_query': query_w.astype(jnp.bfloat16),
        'w_key': key_w.astype(jnp.bfloat16),
        'w_value': draw_matrix(shared_keys[3], MODEL_DIM, MODEL_DIM).astype(jnp.bfloat16),
        'w_out': draw_matrix(shared_keys[4], MODEL_DIM, MODEL_DIM).astype(jnp.bfloat16),
        'norm_mlp': draw_gain(shared_keys[5]),
        'w_gate': draw_matrix(shared_keys[6], MODEL_DIM, FFN_DIM).astype(jnp.bfloat16),
        'w_up': draw_matrix(shared_keys[7], MODEL_DIM, FFN_DIM).astype(jnp.bfloat16),
        'w_down': draw_matrix(shared_keys[8], FFN_DIM, MODEL_DIM).astype(jnp.bfloat16),
    }


def rms_norm(hidden, gain):
    hid_f32 = hidden.astype(jnp.float32)
    inv_rms = lax.rsqrt(jnp.mean(hid_f32 * hid_f32, axis=-1, keepdims=True) + NORM_EPS)
    return (hid_f32 * inv_rms * gain.astype(jnp.float32)).astype(jnp.bfloat16)


def apply_rope(proj, angles):
    half_dim = proj.shape[-1] // 2
    lower_half = proj[..., :half_dim]
    upper_half = proj[..., half_dim:]
    cos_tab = jnp.cos(angles)[..., None, :]
    sin_tab = jnp.sin(angles)[..., None, :]
    return jnp.concatenate([lower_half * cos_tab - upper_half * sin_tab, upper_half * cos_tab + lower_half * sin_tab], axis=-1)


def reference(x_in, norm_attn, w_query, w_key, w_value, w_out, norm_mlp, w_gate, w_up, w_down):
    score_scale = HEAD_DIM ** -0.5
    num_blocks = SEQ_LEN // QUERY_BLOCK
    head_shape = (SEQ_LEN, NUM_HEADS, HEAD_DIM)
    seq_idx = jnp.arange(SEQ_LEN, dtype=jnp.int32)
    row_pos = (seq_idx % SHARD_LEN) * SEQ_SHARDS + seq_idx // SHARD_LEN
    inv_freq = jnp.exp(jnp.arange(HEAD_DIM // 2, dtype=jnp.float32) * (-2.0 * math.log(ROPE_THETA) / HEAD_DIM))
    angles = row_pos.astype(jnp.float32)[:, None] * inv_freq[None, :]
    query_pos = row_pos.reshape(num_blocks, QUERY_BLOCK)

    def row_layer(hidden):
        normed = rms_norm(hidden, norm_attn)
        query_rot = apply_rope(jnp.dot(normed, w_query, preferred_element_type=jnp.float32).reshape(head_shape), angles).astype(jnp.bfloat16)
        key_f32 = apply_rope(jnp.dot(normed, w_key, preferred_element_type=jnp.float32).reshape(head_shape), angles).astype(jnp.bfloat16).astype(jnp.float32)
        value_f32 = jnp.dot(normed, w_value, preferred_element_type=jnp.float32).astype(jnp.bfloat16).astype(jnp.float32).reshape(head_shape)

        def block_layer(block_args):
            hid_blk, query_blk, qpos_blk = block_args
            scores = jnp.einsum('qhd,khd->hqk', query_blk.astype(jnp.float32), key_f32) * score_scale
            allowed = row_pos[None, None, :] <= qpos_blk[None, :, None]
            attn_prob = jax.nn.softmax(jnp.where(allowed, scores, MASK_VALUE), axis=-1)
            attn_mix = jnp.einsum('hqk,khd->qhd', attn_prob, value_f32).astype(jnp.bfloat16).reshape(QUERY_BLOCK, MODEL_DIM)
            resid_blk = (hid_blk.astype(jnp.float32) + jnp.dot(attn_mix, w_out, preferred_element_type=jnp.float32)).astype(jnp.bfloat16)
            normed_mlp = rms_norm(resid_blk, norm_mlp)
            gate_act = jax.nn.silu(jnp.dot(normed_mlp, w_gate, preferred_element_type=jnp.float32))
            up_proj = jnp.dot(normed_mlp, w_up, preferred_element_type=jnp.float32)
            hidden_mlp = (gate_act * up_proj).astype(jnp.bfloat16)
            return (resid_blk.astype(jnp.float32) + jnp.dot(hidden_mlp, w_down, preferred_element_type=jnp.float32)).astype(jnp.bfloat16)

        blocks = (hidden.reshape(num_blocks, QUERY_BLOCK, MODEL_DIM), query_rot.reshape(num_blocks, QUERY_BLOCK, NUM_HEADS, HEAD_DIM), query_pos)
        return lax.map(block_layer, blocks).reshape(SEQ_LEN, MODEL_DIM)

    return lax.map(row_layer, x_in)
```

```python
import math
import functools
import jax
import jax.numpy as jnp
from jax import lax
from jax.experimental import pallas as pl
from jax.experimental.pallas import tpu as pltpu
from jax.sharding import PartitionSpec as P

HEAD = 128
EPS = 1e-5
THETA = 5e7
NEG = -1e30
BF = jnp.bfloat16
F32 = jnp.float32
MESH = pl.DeviceIdType.MESH

D = 4096
HD = D // 2
FFN = 11008
HF = FFN // 2
TOK = 2048
CW = 512
FW = 256

NC, NE, NF, NG = 24, 8, 43, 16
E0 = NC
F0 = E0 + NE
G0 = F0 + NF
N = G0 + NG
NSEM = NC + NE + 2 * NF + NG
DIRECT = 7
C_E, C_M = 256, 512
YAHEAD = 12
SLOTS = 6
KB = 1024
KSPLIT = ((0, 2816), (2816, 5632), (5632, 8448), (8448, FFN))


def kernel(x_in, gown, cos, sin, qpos, kpos, wq, wk, wv, wo, wg, wu, wd,
           y, xr, rq, rk, rv, ro, rg, ru, rd, ob, ubuf, hbuf,
           grem, ys, yr, xs, xrs, dys, dyr, dxs, dxr, gsem, xsend, xrecv, osend, orecv):
    f = lax.axis_index('fsdp')
    s = lax.axis_index('sp')
    cx = s // 2
    cc = s % 2
    ynbr = (0, 1 - f, s)
    xnbr = (0, f, (s + 2) % 4)
    pnbr = (0, f, cx * 2 + 1 - cc)

    def peer(k):
        if k == 1:
            return cx * 2 + 1 - cc
        if k == 2:
            return (s + 2) % 4
        return 3 - s

    bar = pltpu.get_barrier_semaphore()
    for dev in (ynbr, pnbr, xnbr, (0, f, 3 - s)):
        pl.semaphore_signal(bar, inc=1, device_id=dev, device_id_type=MESH)
    pl.semaphore_wait(bar, 4)

    def rcopy(src, dst, ssem, rsem, dev):
        return pltpu.make_async_remote_copy(src_ref=src, dst_ref=dst, send_sem=ssem, recv_sem=rsem, device_id=dev, device_id_type=MESH)

    class Part:
        def __init__(self, w, r, col, ncol, half, e, m, sem):
            self.w, self.r, self.half, self.e, self.m, self.sem = w, r, half, e, m, sem
            self.cols = pl.ds(col, ncol)

        def rows(self, off, n):
            return pl.ds(pl.multiple_of(cc * self.half + off, 32), n)

        def ycopy(self):
            a = (self.rows(cx * self.e, self.e + self.m), self.cols)
            return rcopy(self.w.at[a], self.r.at[a], ys.at[self.sem], yr.at[self.sem], ynbr)

        def xcopy(self):
            a = (self.rows(cx * (self.e + self.m), self.e), self.cols)
            return rcopy(self.r.at[a], self.r.at[a], xs.at[self.sem], xrs.at[self.sem], xnbr)

        def dycopy(self):
            a = (self.rows(cx * self.e, self.e + self.m), self.cols)
            return rcopy(self.r.at[a], self.r.at[a], dys.at[self.sem], dyr.at[self.sem], pnbr)

        def dxcopy(self):
            a = (self.rows((1 - cx) * (self.e + self.m), self.e), self.cols)
            return rcopy(self.r.at[a], self.r.at[a], dxs.at[self.sem], dxr.at[self.sem], pnbr)

        def ysend(self):
            self.ycopy().start()

        def yf(self):
            c = self.ycopy()
            c.wait_recv()
            if self.e:
                self.xcopy().start()
            self.dycopy().start()
            c.wait_send()

        def xf(self):
            if self.e:
                c = self.xcopy()
                c.wait_recv()
                self.dxcopy().start()
                c.wait_send()

        def done(self):
            c = self.dycopy()
            c.wait_recv()
            c.wait_send()
            if self.e:
                c = self.dxcopy()
                c.wait_recv()
                c.wait_send()

    def al(v, k):
        return v if isinstance(v, int) else pl.multiple_of(v, k)

    def when(cond, fn):
        if isinstance(cond, bool):
            if cond:
                fn()
        else:
            pl.when(cond)(fn)

    def item(n, what, cand):
        if 'C' in cand:
            for j, (w, r) in enumerate(((wq, rq), (wk, rk), (wv, rv))):
                col = al((n // 3) * CW, CW)
                if 'D' in cand:
                    when((n < DIRECT) & (n % 3 == j), lambda: getattr(Part(w, r, col, CW, HD // 2, 0, HD // 2, n), what)())
                when((n >= DIRECT) & (n < E0) & (n % 3 == j), lambda: getattr(Part(w, r, col, CW, HD // 2, C_E, C_M, n), what)())
        if 'E' in cand:
            when((n >= E0) & (n < F0), lambda: getattr(Part(wo, ro, al((n - E0) * CW, CW), CW, HD // 2, HD // 4, 0, n), what)())
        if 'F' in cand:
            def both():
                col = al((n - F0) * FW, FW)
                for i, (w, r) in enumerate(((wg, rg), (wu, ru))):
                    getattr(Part(w, r, col, FW, HD // 2, HD // 4, 0, F0 + 2 * (n - F0) + i), what)()
            when((n >= F0) & (n < G0), both)
        if 'G' in cand:
            when((n >= G0) & (n < N), lambda: getattr(Part(wd, rd, al((n - G0) * FW, FW), FW, HF // 2, HF // 4, 0, n + NF), what)())

    gcopy = rcopy(gown, grem, gsem.at[0], gsem.at[1], ynbr)
    gcopy.start()
    for n in range(3):
        item(n, 'ysend', 'CD')

    def xcopy(r, k):
        src = x_in.at[pl.ds(pl.multiple_of((peer(k) * 4 + r) * 128, 128), 128)]
        dst = xr.at[pl.ds(pl.multiple_of(r * 512 + s * 128, 128), 128)]
        return rcopy(src, dst, xsend.at[r, k - 1], xrecv.at[r, k - 1], (0, f, peer(k)))

    for r in range(4):
        for k in (2, 3, 1):
            xcopy(r, k).start()
    for n in range(3, YAHEAD):
        item(n, 'ysend', 'CD')
    gcopy.wait_recv()
    gcopy.wait_send()

    def scope(act, wbuf, obuf, wl, ol):
        def wcopies(n, cand):
            def go(fn):
                slot = n % SLOTS
                if 'C' in cand:
                    for j, (w, r) in enumerate(((wq, rq), (wk, rk), (wv, rv))):
                        a = (slice(None), pl.ds(al((n // 3) * CW, CW), CW))
                        when((n < E0) & (n % 3 == j), lambda: [fn(pltpu.make_async_copy(b.at[a], wbuf.at[slot, i], wl.at[slot, i])) for i, b in enumerate((w, r))] and None)
                if 'E' in cand:
                    a2 = (slice(None), pl.ds(al((n - E0) * CW, CW), CW))
                    when((n >= E0) & (n < F0), lambda: [fn(pltpu.make_async_copy(b.at[a2], wbuf.at[slot, i], wl.at[slot, i])) for i, b in enumerate((wo, ro))] and None)
                if 'F' in cand:
                    a3 = (slice(None), pl.ds(al((n - F0) * FW, FW), FW))

                    def ff():
                        for i, pair in enumerate(((wg, wu), (rg, ru))):
                            for j, b in enumerate(pair):
                                fn(pltpu.make_async_copy(b.at[a3], wbuf.at[slot, i, :, pl.ds(j * FW, FW)], wl.at[slot, i + 2 * j]))
                    when((n >= F0) & (n < G0), ff)
            return go

        def load(n, cand):
            wcopies(n, cand)(lambda c: c.start())

        def loaded(n, cand):
            wcopies(n, cand)(lambda c: c.wait())

        def project(rows, slot):
            acc = None
            for i in range(2):
                for k in range(0, HD, KB):
                    part = jnp.dot(act[i, rows, k:k + KB], wbuf[slot, i, k:k + KB], preferred_element_type=F32)
                    acc = part if acc is None else acc + part
            return acc

        def norm_tile(xt, t, row, g):
            def sub(i, _):
                rs = pl.ds(pl.multiple_of(i * 16, 16), 16)
                x0 = xt[t, 0, rs, :].astype(F32)
                x1 = xt[t, 1, rs, :].astype(F32)
                ss = jnp.sum(x0 * x0, axis=-1, keepdims=True) + jnp.sum(x1 * x1, axis=-1, keepdims=True)
                inv = lax.rsqrt(ss * (1.0 / D) + EPS)
                ro_ = pl.ds(pl.multiple_of(row + i * 16, 16), 16)
                act[0, ro_, :] = (xt[t, 0, rs, :].astype(F32) * inv * gown[pl.ds(g, 1), :]).astype(BF)
                act[1, ro_, :] = (xt[t, 1, rs, :].astype(F32) * inv * grem[pl.ds(g, 1), :]).astype(BF)
                return 0
            lax.fori_loop(0, 8, sub, 0)

        def halves(src, row, xt, t, sem):
            rows = pl.ds(row, 128)
            return [pltpu.make_async_copy(src.at[rows, pl.ds(pl.multiple_of(h * HD, HD), HD)], xt.at[t, i], sem.at[t, i])
                    for i, h in enumerate((f, 1 - f))]

        def attention_phase(xt, xl, qb, kb, vb):
            def tokens(r):
                for k in (1, 2, 3):
                    c = xcopy(r, k)
                    c.wait_recv()
                    c.wait_send()

                def cps(t):
                    return halves(xr, r * 512 + t * 128, xt, t, xl)
                for t in range(4):
                    @pl.when(s != t)
                    def _():
                        for c in cps(t):
                            c.start()

                    @pl.when(s == t)
                    def _():
                        for c in halves(x_in, pl.multiple_of((s * 4 + r) * 128, 128), xt, t, xl):
                            c.start()
                for t in range(4):
                    for c in cps(t):
                        c.wait()
                    norm_tile(xt, t, r * 512 + t * 128, 0)

            def ocopy(g, k):
                src = obuf.at[g % 2, pl.ds(pl.multiple_of(peer(k) * 512, 512), 512)]
                dst = ob.at[pl.ds(pl.multiple_of(s * 512, 512), 512), pl.ds(pl.multiple_of(g * CW, CW), CW)]
                return rcopy(src, dst, osend.at[g, k - 1], orecv.at[g, k - 1], (0, f, peer(k)))

            def olocal(g):
                return pltpu.make_async_copy(obuf.at[g % 2, pl.ds(pl.multiple_of(s * 512, 512), 512)],
                                             ob.at[pl.ds(pl.multiple_of(s * 512, 512), 512), pl.ds(pl.multiple_of(g * CW, CW), CW)], ol.at[g % 2])

            def rope(acc):
                out = []
                for h in range(CW // HEAD):
                    u = acc[:, h * HEAD:(h + 1) * HEAD]
                    out.append(u * cos[...] + pltpu.roll(u, HEAD // 2, 1) * sin[...])
                return jnp.concatenate(out, axis=1).astype(BF)

            def unit(q, _):
                g, r = q // 4, q % 4
                rows = pl.ds(pl.multiple_of(r * 512, 512), 512)

                @pl.when(r == 0)
                def _():
                    for j in range(3):
                        loaded(3 * g + j, 'C')

                    @pl.when(g >= 2)
                    def _():
                        for k in (1, 2, 3):
                            ocopy(g - 2, k).wait_send()
                        olocal(g - 2).wait()

                @pl.when(g == 0)
                def _():
                    tokens(r)

                base = (g % 2) * 3
                for j, (dst, fn) in enumerate(((qb, rope), (kb, rope), (vb, lambda a: a.astype(BF)))):
                    acc = project(rows, base + j)
                    dst[...] = fn(acc)

                def head(h, _):
                    hs = pl.ds(pl.multiple_of(h * HEAD, HEAD), HEAD)
                    sc = lax.dot_general(qb[:, hs], kb[:, hs], (((1,), (1,)), ((), ())), preferred_element_type=F32)
                    qp = qpos[...]
                    sc = jnp.where(jnp.concatenate([qp] * 4, axis=1) >= kpos[...], sc, NEG)
                    mx = jnp.max(sc, axis=-1, keepdims=True)
                    p = jnp.exp2((sc - mx) * (HEAD ** -0.5 * math.log2(math.e)))
                    tot = jnp.sum(p, axis=-1, keepdims=True)
                    o = jnp.dot(p.astype(BF), vb[:, hs], preferred_element_type=F32) / tot
                    o = o.astype(BF)
                    for t in range(4):
                        obuf[g % 2, pl.ds(pl.multiple_of(t * 512 + r * 128, 128), 128), hs] = o[t * 128:(t + 1) * 128]
                    return 0
                lax.fori_loop(0, CW // HEAD, head, 0)

                for qq, (yy, dd) in {0: ((3,), ()), 1: ((4,), (3,)), 2: ((5, 6, 7), (4,)), 3: ((8,), (5,))}.items():
                    @pl.when(q == qq)
                    def _():
                        for n in yy:
                            item(n, 'yf', 'CD')
                            item(n + YAHEAD - 3, 'ysend', 'CD')
                        for n in dd:
                            item(n, 'done', 'CD')
                            load(n, 'C')

                @pl.when((q >= 4) & (r < 3))
                def _():
                    n = 3 * g + 3 + r
                    item(n + YAHEAD, 'ysend', 'CEF')
                    item(n + 3, 'yf', 'CEF')
                    item(n + 1, 'xf', 'CE')
                    item(n, 'done', 'CDE')
                    load(n, 'CE')

                @pl.when(r == 3)
                def _():
                    for k in (2, 3, 1):
                        ocopy(g, k).start()
                    olocal(g).start()
                return 0

            for n in range(3):
                item(n, 'yf', 'CD')
                item(n, 'done', 'CD')
                load(n, 'C')
            lax.fori_loop(0, 32, unit, 0)
            for g in (6, 7):
                for k in (1, 2, 3):
                    ocopy(g, k).wait_send()
                olocal(g).wait()

            def arrived(g, _):
                for k in (1, 2, 3):
                    ocopy(g, k).wait_recv()
                return 0
            lax.fori_loop(0, 8, arrived, 0)

        pl.run_scoped(attention_phase, pltpu.VMEM((4, 2, 128, HD), BF), pltpu.SemaphoreType.DMA((4, 2)),
                      pltpu.VMEM((512, CW), BF), pltpu.VMEM((512, CW), BF), pltpu.VMEM((512, CW), BF))

        MT = 1024

        def out_phase(hx, hl, al_):
            def acopy(t, i):
                h = f if i == 0 else 1 - f
                rows = pl.ds(t * MT, MT)
                return pltpu.make_async_copy(ob.at[rows, pl.ds(pl.multiple_of(h * HD, HD), HD)], act.at[i, rows], al_.at[t, i])
            for t in range(TOK // MT):
                for i in range(2):
                    acopy(t, i).start()

            def xload(n):
                return pltpu.make_async_copy(x_in.at[:, pl.ds(pl.multiple_of((n - E0) * CW, CW), CW)], hx.at[n % 2], hl.at[n % 2])

            def hstore(n):
                return pltpu.make_async_copy(obuf.at[n % 2], hbuf.at[:, pl.ds(pl.multiple_of((n - E0) * CW, CW), CW)], ol.at[n % 2])

            xload(jnp.int32(E0)).start()
            for t in range(TOK // MT):
                for i in range(2):
                    acopy(t, i).wait()

            def step(n, _):
                item(n + YAHEAD + 3, 'ysend', 'EF')
                item(n + 6, 'yf', 'EF')
                item(n + 4, 'xf', 'EF')
                item(n + 3, 'done', 'EF')
                load(n + 3, 'EF')

                @pl.when(n + 1 < F0)
                def _():
                    xload(n + 1).start()

                @pl.when(n >= E0 + 2)
                def _():
                    hstore(n - 2).wait()
                loaded(n, 'E')
                xload(n).wait()
                slot = n % SLOTS

                def mt(t, _):
                    rows = pl.ds(pl.multiple_of(t * MT, MT), MT)
                    acc = project(rows, slot)
                    obuf[n % 2, rows, :] = (hx[n % 2, rows, :].astype(F32) + acc).astype(BF)
                    return 0
                lax.fori_loop(0, TOK // MT, mt, 0)
                hstore(n).start()
                return 0
            lax.fori_loop(E0, F0, step, 0)
            for n in (F0 - 2, F0 - 1):
                hstore(jnp.int32(n)).wait()

        pl.run_scoped(out_phase, pltpu.VMEM((2, TOK, CW), BF), pltpu.SemaphoreType.DMA((2,)), pltpu.SemaphoreType.DMA((2, 2)))

        def norm_phase(xt, xl):
            def cps(i):
                return halves(hbuf, pl.multiple_of(i * 128, 128), xt, i % 4, xl)
            for i in range(3):
                for c in cps(jnp.int32(i)):
                    c.start()

            def step(i, _):
                @pl.when(i + 3 < 16)
                def _():
                    for c in cps(i + 3):
                        c.start()
                for c in cps(i):
                    c.wait()
                norm_tile(xt, i % 4, i * 128, 1)
                return 0
            lax.fori_loop(0, 16, step, 0)

        pl.run_scoped(norm_phase, pltpu.VMEM((4, 2, 128, HD), BF), pltpu.SemaphoreType.DMA((4, 2)))

        def ustore(n):
            return pltpu.make_async_copy(obuf.at[n % 2, :, pl.ds(0, FW)], ubuf.at[:, pl.ds(pl.multiple_of((n - F0) * FW, FW), FW)], ol.at[n % 2])

        def gate_step(n, _):
            item(n + YAHEAD + 3, 'ysend', 'FG')
            item(n + 6, 'yf', 'FG')
            item(n + 4, 'xf', 'FG')
            item(n + 3, 'done', 'FG')
            load(n + 3, 'F')

            @pl.when(n >= F0 + 2)
            def _():
                ustore(n - 2).wait()
            loaded(n, 'F')
            slot = n % SLOTS

            def mt(t, _):
                rows = pl.ds(pl.multiple_of(t * MT, MT), MT)
                acc = project(rows, slot)
                gate, up = acc[:, :FW], acc[:, FW:]
                obuf[n % 2, rows, pl.ds(0, FW)] = (gate * jax.nn.sigmoid(gate) * up).astype(BF)
                return 0
            lax.fori_loop(0, TOK // MT, mt, 0)
            ustore(n).start()
            return 0
        lax.fori_loop(F0, G0, gate_step, 0)
        for n in (G0 - 2, G0 - 1):
            ustore(jnp.int32(n)).wait()

    pl.run_scoped(scope, pltpu.VMEM((2, TOK, HD), BF), pltpu.VMEM((SLOTS, 2, HD, CW), BF), pltpu.VMEM((2, TOK, CW), BF),
                  pltpu.SemaphoreType.DMA((SLOTS, 4)), pltpu.SemaphoreType.DMA((2,)))

    MD = 512

    def down_phase(u, wbuf, hb, yb, ul, wl, hl, yl):
        def ucopy(t):
            rows = pl.ds(t * MD, MD)
            return pltpu.make_async_copy(ubuf.at[rows], u.at[rows], ul.at[t])

        def wcopies(n):
            cols = pl.ds(pl.multiple_of((n - G0) * FW, FW), FW)
            return [pltpu.make_async_copy(b.at[:, cols], wbuf.at[n % 2, pl.ds(pl.multiple_of(h * HF, 128), HF)], wl.at[n % 2, i])
                    for i, (b, h) in enumerate(((wd, f), (rd, 1 - f)))]

        tiles = TOK // MD

        def at(q):
            return pl.ds(pl.multiple_of((q % tiles) * MD, MD), MD), pl.ds(pl.multiple_of((q // tiles) * FW, FW), FW)

        def hcopy(q):
            return pltpu.make_async_copy(hbuf.at[at(q)], hb.at[q % 2], hl.at[q % 2])

        def ycopy(q):
            return pltpu.make_async_copy(yb.at[q % 2], y.at[at(q)], yl.at[q % 2])

        for t in range(TOK // MD):
            ucopy(t).start()
            if t == 0:
                for c in wcopies(jnp.int32(G0)):
                    c.start()
                hcopy(jnp.int32(0)).start()

        def step(n, _):
            item(n + YAHEAD + 3, 'ysend', 'G')

            @pl.when(n + 3 >= G0 + 6)
            def _():
                item(n + 3, 'yf', 'G')

            @pl.when(n + 2 >= G0 + 4)
            def _():
                item(n + 2, 'xf', 'G')

            @pl.when(n + 1 >= G0 + 3)
            def _():
                item(n + 1, 'done', 'G')

            @pl.when(n + 1 < N)
            def _():
                for c in wcopies(n + 1):
                    c.start()
            for c in wcopies(n):
                c.wait()

            def mt(t, _):
                rows = pl.ds(pl.multiple_of(t * MD, MD), MD)
                q = (n - G0) * tiles + t

                @pl.when(n == G0)
                def _():
                    pltpu.make_async_copy(ubuf.at[rows], u.at[rows], ul.at[t]).wait()

                @pl.when(q + 1 < NG * tiles)
                def _():
                    hcopy(q + 1).start()

                @pl.when(q >= 2)
                def _():
                    ycopy(q - 2).wait()
                hcopy(q).wait()
                acc = None
                for a, b in KSPLIT:
                    part = jnp.dot(u[rows, a:b], wbuf[n % 2, a:b], preferred_element_type=F32)
                    acc = part if acc is None else acc + part
                yb[q % 2] = (hb[q % 2].astype(F32) + acc).astype(BF)
                ycopy(q).start()
                return 0
            lax.fori_loop(0, tiles, mt, 0)
            return 0
        lax.fori_loop(G0, N, step, 0)
        for q in (NG * tiles - 2, NG * tiles - 1):
            ycopy(jnp.int32(q)).wait()

    pl.run_scoped(down_phase, pltpu.VMEM((TOK, FFN), BF), pltpu.VMEM((2, FFN, FW), BF), pltpu.VMEM((2, MD, FW), BF), pltpu.VMEM((2, MD, FW), BF),
                  pltpu.SemaphoreType.DMA((TOK // MD,)), pltpu.SemaphoreType.DMA((2, 2)), pltpu.SemaphoreType.DMA((2,)), pltpu.SemaphoreType.DMA((2,)))


def local_layer(x_loc, norm_attn, w_query, w_key, w_value, w_out, norm_mlp, w_gate, w_up, w_down):
    shape = x_loc.shape
    x2 = x_loc.reshape(TOK, D)
    gains = jnp.stack([norm_attn, norm_mlp]).astype(F32)
    idx = jnp.arange(512, dtype=jnp.int32)
    pos = (idx % 128) * 4 + idx // 128
    inv_freq = jnp.exp(jnp.arange(HEAD // 2, dtype=F32) * (-2.0 * math.log(THETA) / HEAD))
    ang = pos.astype(F32)[:, None] * inv_freq[None, :]
    cos, sin = jnp.cos(ang), jnp.sin(ang)
    cos = jnp.concatenate([cos, cos], axis=1)
    sin = jnp.concatenate([-sin, sin], axis=1)
    qpos = jnp.broadcast_to(pos[:, None], (512, 128))
    kpos = pos[None, :]
    anys = pl.BlockSpec(memory_space=pl.ANY)
    vm = pl.BlockSpec(memory_space=pltpu.VMEM)

    def out(*sh):
        return jax.ShapeDtypeStruct(sh, BF)
    sem = pltpu.SemaphoreType.DMA
    res = pl.pallas_call(
        kernel,
        out_shape=[out(TOK, D), out(TOK, D), out(HD, D), out(HD, D), out(HD, D), out(HD, D), out(HD, FFN), out(HD, FFN), out(HF, D),
                   out(TOK, D), out(TOK, FFN), out(TOK, D)],
        in_specs=[anys, vm, vm, vm, vm, vm] + [anys] * 7,
        out_specs=[anys] * 12,
        scratch_shapes=[pltpu.VMEM((2, HD), F32)] + [sem((NSEM,))] * 8 + [sem((2,)), sem((4, 3)), sem((4, 3)), sem((8, 3)), sem((8, 3))],
        compiler_params=pltpu.CompilerParams(collective_id=0, has_side_effects=True, vmem_limit_bytes=66_900_000),
        cost_estimate=pl.CostEstimate(flops=846 * 10**9, bytes_accessed=10**9, transcendentals=0),
        name='layer',
    )(x2, gains, cos, sin, qpos, kpos, w_query, w_key, w_value, w_out, w_gate, w_up, w_down)
    return res[0].reshape(shape)


def solution(mesh):
    rows = P(('dp', 'fsdp'), 'sp', None)
    weight = P('fsdp', None)
    gain = P('fsdp')
    specs = (rows, gain, weight, weight, weight, weight, gain, weight, weight, weight)
    return jax.shard_map(local_layer, mesh=mesh, in_specs=specs, out_specs=rows, check_vma=False)
```

```python
import math
import functools
import jax
import jax.numpy as jnp
from jax import lax
from jax.experimental import pallas as pl
from jax.experimental.pallas import tpu as pltpu
from jax.sharding import PartitionSpec as P

HEAD = 128
EPS = 1e-5
THETA = 5e7
NEG = -1e30
BF = jnp.bfloat16
F32 = jnp.float32
MESH = pl.DeviceIdType.MESH

D = 4096
HD = D // 2
FFN = 11008
HF = FFN // 2
TOK = 2048
CW = 512
FW = 256

NC, NE, NF, NG = 24, 8, 43, 16
E0 = NC
F0 = E0 + NE
G0 = F0 + NF
N = G0 + NG
NSEM = NC + NE + 2 * NF + NG
DIRECT = 7
C_E = 352
E_E = 512
F_E = 512
G_E = 1216
YAHEAD = 14
SLOTS = 6
KB = 1024
KSPLIT = ((0, 2816), (2816, 5632), (5632, 8448), (8448, FFN))


def kernel(x_in, gattn, gmlp, wq, wk, wv, wo, wg, wu, wd,
           y, xr, rq, rk, rv, ro, rg, ru, rd, ob, ubuf, hbuf,
           gown, grem, gains, cos, sin, qpos, ys, yr, xs, xrs, dys, dyr, dxs, dxr, gsem, xsend, xrecv, osend, orecv):
    f = lax.axis_index('fsdp')
    s = lax.axis_index('sp')
    cx = s // 2
    cc = s % 2
    ynbr = (0, 1 - f, s)
    xnbr = (0, f, (s + 2) % 4)
    pnbr = (0, f, cx * 2 + 1 - cc)

    def peer(k):
        if k == 1:
            return cx * 2 + 1 - cc
        if k == 2:
            return (s + 2) % 4
        return 3 - s

    bar = pltpu.get_barrier_semaphore()
    for dev in (ynbr, pnbr, xnbr, (0, f, 3 - s)):
        pl.semaphore_signal(bar, inc=1, device_id=dev, device_id_type=MESH)
    pl.semaphore_wait(bar, 4)

    def rcopy(src, dst, ssem, rsem, dev):
        return pltpu.make_async_remote_copy(src_ref=src, dst_ref=dst, send_sem=ssem, recv_sem=rsem, device_id=dev, device_id_type=MESH)

    class Part:
        def __init__(self, w, r, col, ncol, half, e, sem):
            self.w, self.r, self.half, self.e, self.m, self.sem = w, r, half, e, half - 2 * e, sem
            self.cols = pl.ds(col, ncol)

        def rows(self, off, n):
            return pl.ds(pl.multiple_of(cc * self.half + off, 16), n)

        def ycopy(self):
            a = (self.rows(cx * self.e, self.e + self.m), self.cols)
            return rcopy(self.w.at[a], self.r.at[a], ys.at[self.sem], yr.at[self.sem], ynbr)

        def xcopy(self):
            a = (self.rows(cx * (self.e + self.m), self.e), self.cols)
            return rcopy(self.r.at[a], self.r.at[a], xs.at[self.sem], xrs.at[self.sem], xnbr)

        def dycopy(self):
            a = (self.rows(cx * self.e, self.e + self.m), self.cols)
            return rcopy(self.r.at[a], self.r.at[a], dys.at[self.sem], dyr.at[self.sem], pnbr)

        def dxcopy(self):
            a = (self.rows((1 - cx) * (self.e + self.m), self.e), self.cols)
            return rcopy(self.r.at[a], self.r.at[a], dxs.at[self.sem], dxr.at[self.sem], pnbr)

        def ysend(self):
            self.ycopy().start()

        def yf(self):
            c = self.ycopy()
            c.wait_recv()
            if self.e:
                self.xcopy().start()
            self.dycopy().start()
            c.wait_send()

        def xf(self):
            if self.e:
                c = self.xcopy()
                c.wait_recv()
                self.dxcopy().start()
                c.wait_send()

        def done(self):
            c = self.dycopy()
            c.wait_recv()
            c.wait_send()
            if self.e:
                c = self.dxcopy()
                c.wait_recv()
                c.wait_send()

    def al(v, k):
        return v if isinstance(v, int) else pl.multiple_of(v, k)

    def when(cond, fn):
        if isinstance(cond, bool):
            if cond:
                fn()
        else:
            pl.when(cond)(fn)

    def item(n, what, cand):
        if 'C' in cand:
            for j, (w, r) in enumerate(((wq, rq), (wk, rk), (wv, rv))):
                col = al((n // 3) * CW, CW)
                if 'D' in cand:
                    when((n < DIRECT) & (n % 3 == j), lambda: getattr(Part(w, r, col, CW, HD // 2, 0, n), what)())
                when((n >= DIRECT) & (n < E0) & (n % 3 == j), lambda: getattr(Part(w, r, col, CW, HD // 2, C_E, n), what)())
        if 'E' in cand:
            when((n >= E0) & (n < F0), lambda: getattr(Part(wo, ro, al((n - E0) * CW, CW), CW, HD // 2, E_E, n), what)())
        if 'F' in cand:
            def both():
                col = al((n - F0) * FW, FW)
                for i, (w, r) in enumerate(((wg, rg), (wu, ru))):
                    getattr(Part(w, r, col, FW, HD // 2, F_E, F0 + 2 * (n - F0) + i), what)()
            when((n >= F0) & (n < G0), both)
        if 'G' in cand:
            when((n >= G0) & (n < N), lambda: getattr(Part(wd, rd, al((n - G0) * FW, FW), FW, HF // 2, G_E, n + NF), what)())

    gown[0] = gattn[...].astype(F32)
    gown[1] = gmlp[...].astype(F32)
    gcopy = rcopy(gown, grem, gsem.at[0], gsem.at[1], ynbr)
    gcopy.start()
    for n in range(3):
        item(n, 'ysend', 'CD')

    def xcopy(r, k):
        src = x_in.at[pl.ds(pl.multiple_of((peer(k) * 4 + r) * 128, 128), 128)]
        dst = xr.at[pl.ds(pl.multiple_of(r * 512 + s * 128, 128), 128)]
        return rcopy(src, dst, xsend.at[r, k - 1], xrecv.at[r, k - 1], (0, f, peer(k)))

    for r in range(4):
        for k in (2, 3, 1):
            xcopy(r, k).start()
    for n in range(3, YAHEAD):
        item(n, 'ysend', 'CD')

    def positions(shape, dim):
        j = lax.broadcasted_iota(jnp.int32, shape, dim)
        return (j % 128) * 4 + j // 128

    def table(i, _):
        rs = pl.ds(pl.multiple_of(i * 128, 128), 128)
        pos = lax.broadcasted_iota(jnp.int32, (128, HEAD), 0) * 4 + i
        lane = lax.broadcasted_iota(jnp.int32, (128, HEAD), 1)
        freq = jnp.exp((lane % (HEAD // 2)).astype(F32) * (-2.0 * math.log(THETA) / HEAD))
        ang = pos.astype(F32) * freq
        qpos[rs, :] = pos
        cos[rs, :] = jnp.cos(ang)
        sn = jnp.sin(ang)
        sin[rs, :] = jnp.where(lane < HEAD // 2, -sn, sn)
        return 0
    lax.fori_loop(0, 4, table, 0)
    gcopy.wait_recv()
    gcopy.wait_send()
    for g in range(2):
        for i, src in enumerate((gown, grem)):
            v = src[g]
            gains[2 * g + i] = jnp.concatenate([v[k:k + 1] for k in range(HD // 128)], axis=1)

    def scope(act, wbuf, obuf, wl, ol):
        def wcopies(n, cand):
            def go(fn):
                slot = n % SLOTS
                if 'C' in cand:
                    for j, (w, r) in enumerate(((wq, rq), (wk, rk), (wv, rv))):
                        a = (slice(None), pl.ds(al((n // 3) * CW, CW), CW))
                        when((n < E0) & (n % 3 == j), lambda: [fn(pltpu.make_async_copy(b.at[a], wbuf.at[slot, i], wl.at[slot, i])) for i, b in enumerate((w, r))] and None)
                if 'E' in cand:
                    a2 = (slice(None), pl.ds(al((n - E0) * CW, CW), CW))
                    when((n >= E0) & (n < F0), lambda: [fn(pltpu.make_async_copy(b.at[a2], wbuf.at[slot, i], wl.at[slot, i])) for i, b in enumerate((wo, ro))] and None)
                if 'F' in cand:
                    a3 = (slice(None), pl.ds(al((n - F0) * FW, FW), FW))

                    def ff():
                        for i, pair in enumerate(((wg, wu), (rg, ru))):
                            for j, b in enumerate(pair):
                                fn(pltpu.make_async_copy(b.at[a3], wbuf.at[slot, i, :, pl.ds(j * FW, FW)], wl.at[slot, i + 2 * j]))
                    when((n >= F0) & (n < G0), ff)
            return go

        def load(n, cand):
            wcopies(n, cand)(lambda c: c.start())

        def loaded(n, cand):
            wcopies(n, cand)(lambda c: c.wait())

        def project(rows, slot):
            acc = None
            for i in range(2):
                for k in range(0, HD, KB):
                    part = jnp.dot(act[i, rows, k:k + KB], wbuf[slot, i, k:k + KB], preferred_element_type=F32)
                    acc = part if acc is None else acc + part
            return acc

        def norm_tile(xt, t, row, g):
            def sub(i, _):
                rs = pl.ds(pl.multiple_of(i * 16, 16), 16)
                x0 = xt[t, 0, rs, :].astype(F32)
                x1 = xt[t, 1, rs, :].astype(F32)
                ss = jnp.sum(x0 * x0, axis=-1, keepdims=True) + jnp.sum(x1 * x1, axis=-1, keepdims=True)
                inv = lax.rsqrt(ss * (1.0 / D) + EPS)
                ro_ = pl.ds(pl.multiple_of(row + i * 16, 16), 16)
                act[0, ro_, :] = (xt[t, 0, rs, :].astype(F32) * inv * gains[2 * g]).astype(BF)
                act[1, ro_, :] = (xt[t, 1, rs, :].astype(F32) * inv * gains[2 * g + 1]).astype(BF)
                return 0
            lax.fori_loop(0, 8, sub, 0)

        def halves(src, row, xt, t, sem):
            rows = pl.ds(row, 128)
            return [pltpu.make_async_copy(src.at[rows, pl.ds(pl.multiple_of(h * HD, HD), HD)], xt.at[t, i], sem.at[t, i])
                    for i, h in enumerate((f, 1 - f))]

        def attention_phase(xt, xl, qb, kb, vb):
            def tokens(r):
                for k in (1, 2, 3):
                    c = xcopy(r, k)
                    c.wait_recv()
                    c.wait_send()

                def cps(t):
                    return halves(xr, r * 512 + t * 128, xt, t, xl)
                for t in range(4):
                    @pl.when(s != t)
                    def _():
                        for c in cps(t):
                            c.start()

                    @pl.when(s == t)
                    def _():
                        for c in halves(x_in, pl.multiple_of((s * 4 + r) * 128, 128), xt, t, xl):
                            c.start()
                for t in range(4):
                    for c in cps(t):
                        c.wait()
                    norm_tile(xt, t, r * 512 + t * 128, 0)

            def ocopy(g, k):
                src = obuf.at[g % 2, pl.ds(pl.multiple_of(peer(k) * 512, 512), 512)]
                dst = ob.at[pl.ds(pl.multiple_of(s * 512, 512), 512), pl.ds(pl.multiple_of(g * CW, CW), CW)]
                return rcopy(src, dst, osend.at[g, k - 1], orecv.at[g, k - 1], (0, f, peer(k)))

            def orow(g, k, r):
                src = obuf.at[g % 2, pl.ds(pl.multiple_of(peer(k) * 512 + r * 128, 128), 128)]
                dst = ob.at[pl.ds(pl.multiple_of(s * 512 + r * 128, 128), 128), pl.ds(pl.multiple_of(g * CW, CW), CW)]
                return rcopy(src, dst, osend.at[g, k - 1], orecv.at[g, k - 1], (0, f, peer(k)))

            def olocal(g):
                return pltpu.make_async_copy(obuf.at[g % 2, pl.ds(pl.multiple_of(s * 512, 512), 512)],
                                             ob.at[pl.ds(pl.multiple_of(s * 512, 512), 512), pl.ds(pl.multiple_of(g * CW, CW), CW)], ol.at[g % 2])

            def rope(acc):
                out = []
                for h in range(CW // HEAD):
                    u = acc[:, h * HEAD:(h + 1) * HEAD]
                    out.append(u * cos[...] + pltpu.roll(u, HEAD // 2, 1) * sin[...])
                return jnp.concatenate(out, axis=1).astype(BF)

            def unit(q, _):
                g, r = q // 4, q % 4
                rows = pl.ds(pl.multiple_of(r * 512, 512), 512)

                @pl.when(r == 0)
                def _():
                    for j in range(3):
                        loaded(3 * g + j, 'C')

                    @pl.when(g >= 2)
                    def _():
                        for k in (1, 2, 3):
                            ocopy(g - 2, k).wait_send()
                        olocal(g - 2).wait()

                @pl.when(g == 0)
                def _():
                    tokens(r)

                base = (g % 2) * 3
                for j, (dst, fn) in enumerate(((qb, rope), (kb, rope), (vb, lambda a: a.astype(BF)))):
                    acc = project(rows, base + j)
                    dst[...] = fn(acc)

                def head(h, _):
                    hs = pl.ds(pl.multiple_of(h * HEAD, HEAD), HEAD)
                    sc = lax.dot_general(qb[:, hs], kb[:, hs], (((1,), (1,)), ((), ())), preferred_element_type=F32)
                    qp = qpos[...]
                    kp = positions((1, 512), 1)
                    sc = jnp.where(jnp.concatenate([qp] * 4, axis=1) >= kp, sc, NEG)
                    mx = jnp.max(sc, axis=-1, keepdims=True)
                    p = jnp.exp2((sc - mx) * (HEAD ** -0.5 * math.log2(math.e)))
                    tot = jnp.sum(p, axis=-1, keepdims=True)
                    o = jnp.dot(p.astype(BF), vb[:, hs], preferred_element_type=F32) / tot
                    o = o.astype(BF)
                    for t in range(4):
                        obuf[g % 2, pl.ds(pl.multiple_of(t * 512 + r * 128, 128), 128), hs] = o[t * 128:(t + 1) * 128]
                    return 0
                lax.fori_loop(0, CW // HEAD, head, 0)

                for k in (2, 3, 1):
                    orow(g, k, r).start()

                @pl.when(r == 3)
                def _():
                    olocal(g).start()
                for qq, (yy, dd) in {0: ((3,), ()), 1: ((4,), (3,)), 2: ((5, 6, 7), (4,)), 3: ((8,), (5,))}.items():
                    @pl.when(q == qq)
                    def _():
                        for n in yy:
                            item(n, 'yf', 'CD')
                            item(n + YAHEAD - 3, 'ysend', 'CD')
                        for n in dd:
                            item(n, 'done', 'CD')
                            load(n, 'C')

                @pl.when((q >= 4) & (r < 3))
                def _():
                    n = 3 * g + 3 + r
                    item(n + YAHEAD, 'ysend', 'CEF')

                    @pl.when(g < 7)
                    def _():
                        item(n + 3, 'yf', 'CE')
                        item(n + 1, 'xf', 'CE')
                        item(n, 'done', 'CD')
                        load(n, 'C')
                return 0

            for n in range(3):
                item(n, 'yf', 'CD')
                item(n, 'done', 'CD')
                load(n, 'C')
            lax.fori_loop(0, 32, unit, 0)
            for n in range(E0 + 3, E0 + 6):
                item(n, 'yf', 'E')
            for n in range(E0, E0 + 3):
                item(n + 1, 'xf', 'E')
                item(n, 'done', 'E')
                load(n, 'E')
            for g in (6, 7):
                for k in (1, 2, 3):
                    ocopy(g, k).wait_send()
                olocal(g).wait()

            def arrived(g, _):
                for k in (1, 2, 3):
                    ocopy(g, k).wait_recv()
                return 0
            lax.fori_loop(0, 8, arrived, 0)

        pl.run_scoped(attention_phase, pltpu.VMEM((4, 2, 128, HD), BF), pltpu.SemaphoreType.DMA((4, 2)),
                      pltpu.VMEM((512, CW), BF), pltpu.VMEM((512, CW), BF), pltpu.VMEM((512, CW), BF))

        MT = 1024

        def out_phase(hx, hl, al_):
            def acopy(t, i):
                h = f if i == 0 else 1 - f
                rows = pl.ds(t * MT, MT)
                return pltpu.make_async_copy(ob.at[rows, pl.ds(pl.multiple_of(h * HD, HD), HD)], act.at[i, rows], al_.at[t, i])
            for t in range(TOK // MT):
                for i in range(2):
                    acopy(t, i).start()

            def xload(n):
                return pltpu.make_async_copy(x_in.at[:, pl.ds(pl.multiple_of((n - E0) * CW, CW), CW)], hx.at[n % 2], hl.at[n % 2])

            def hstore(n):
                return pltpu.make_async_copy(obuf.at[n % 2], hbuf.at[:, pl.ds(pl.multiple_of((n - E0) * CW, CW), CW)], ol.at[n % 2])

            xload(jnp.int32(E0)).start()
            for t in range(TOK // MT):
                for i in range(2):
                    acopy(t, i).wait()

            def step(n, _):
                item(n + YAHEAD + 3, 'ysend', 'EF')
                @pl.when(n + 5 >= E0 + 6)
                def _():
                    item(n + 5, 'yf', 'EF')

                @pl.when(n + 2 >= E0 + 4)
                def _():
                    item(n + 2, 'xf', 'EF')
                    item(n + 1, 'done', 'EF')
                    load(n + 1, 'EF')

                @pl.when(n + 1 < F0)
                def _():
                    xload(n + 1).start()

                @pl.when(n >= E0 + 2)
                def _():
                    hstore(n - 2).wait()
                loaded(n, 'E')
                xload(n).wait()
                slot = n % SLOTS

                def mt(t, _):
                    rows = pl.ds(pl.multiple_of(t * MT, MT), MT)
                    acc = project(rows, slot)
                    obuf[n % 2, rows, :] = (hx[n % 2, rows, :].astype(F32) + acc).astype(BF)
                    return 0
                lax.fori_loop(0, TOK // MT, mt, 0)
                hstore(n).start()
                return 0
            lax.fori_loop(E0, F0, step, 0)
            for n in (F0 - 2, F0 - 1):
                hstore(jnp.int32(n)).wait()

        pl.run_scoped(out_phase, pltpu.VMEM((2, TOK, CW), BF), pltpu.SemaphoreType.DMA((2,)), pltpu.SemaphoreType.DMA((2, 2)))

        def norm_phase(xt, xl):
            def cps(i):
                return halves(hbuf, pl.multiple_of(i * 128, 128), xt, i % 4, xl)
            for i in range(3):
                for c in cps(jnp.int32(i)):
                    c.start()

            def step(i, _):
                @pl.when(i + 3 < 16)
                def _():
                    for c in cps(i + 3):
                        c.start()
                for c in cps(i):
                    c.wait()
                norm_tile(xt, i % 4, i * 128, 1)
                return 0
            lax.fori_loop(0, 16, step, 0)

        pl.run_scoped(norm_phase, pltpu.VMEM((4, 2, 128, HD), BF), pltpu.SemaphoreType.DMA((4, 2)))

        def ustore(n):
            return pltpu.make_async_copy(obuf.at[n % 2, :, pl.ds(0, FW)], ubuf.at[:, pl.ds(pl.multiple_of((n - F0) * FW, FW), FW)], ol.at[n % 2])

        def gate_step(n, _):
            item(n + YAHEAD + 3, 'ysend', 'FG')
            item(n + 5, 'yf', 'FG')
            item(n + 2, 'xf', 'FG')
            item(n + 1, 'done', 'FG')
            load(n + 1, 'F')

            @pl.when(n >= F0 + 2)
            def _():
                ustore(n - 2).wait()
            loaded(n, 'F')
            slot = n % SLOTS

            def mt(t, _):
                rows = pl.ds(pl.multiple_of(t * MT, MT), MT)
                acc = project(rows, slot)
                gate, up = acc[:, :FW], acc[:, FW:]
                obuf[n % 2, rows, pl.ds(0, FW)] = (gate * jax.nn.sigmoid(gate) * up).astype(BF)
                return 0
            lax.fori_loop(0, TOK // MT, mt, 0)
            ustore(n).start()
            return 0
        lax.fori_loop(F0, G0, gate_step, 0)
        for n in (G0 - 2, G0 - 1):
            ustore(jnp.int32(n)).wait()

    pl.run_scoped(scope, pltpu.VMEM((2, TOK, HD), BF), pltpu.VMEM((SLOTS, 2, HD, CW), BF), pltpu.VMEM((2, TOK, CW), BF),
                  pltpu.SemaphoreType.DMA((SLOTS, 4)), pltpu.SemaphoreType.DMA((2,)))

    MD = 512

    def down_phase(u, wbuf, hb, yb, ul, wl, hl, yl):
        def ucopy(t):
            rows = pl.ds(pl.multiple_of(t * MD, MD), MD)
            return pltpu.make_async_copy(ubuf.at[rows], u.at[rows], ul.at[t])

        def wcopy(n, i):
            cols = pl.ds(pl.multiple_of((n - G0) * FW, FW), FW)
            h = (f, 1 - f)[i]
            return pltpu.make_async_copy((wd, rd)[i].at[:, cols], wbuf.at[n % 2, pl.ds(pl.multiple_of(h * HF, 128), HF)], wl.at[n % 2, i])

        tiles = TOK // MD

        def at(q):
            return pl.ds(pl.multiple_of((q % tiles) * MD, MD), MD), pl.ds(pl.multiple_of((q // tiles) * FW, FW), FW)

        def hcopy(q):
            return pltpu.make_async_copy(hbuf.at[at(q)], hb.at[q % 2], hl.at[q % 2])

        def ycopy(q):
            return pltpu.make_async_copy(yb.at[q % 2], y.at[at(q)], yl.at[q % 2])

        for t in range(tiles):
            ucopy(t).start()
            if t == 0:
                for i in range(2):
                    wcopy(jnp.int32(G0), i).start()
                hcopy(jnp.int32(0)).start()

        def step(n, _):
            item(n + YAHEAD + 3, 'ysend', 'G')

            @pl.when(n + 4 >= G0 + 5)
            def _():
                item(n + 4, 'yf', 'G')
            item(n + 2, 'xf', 'G')
            item(n + 1, 'done', 'G')

            @pl.when(n + 1 < N)
            def _():
                for i in range(2):
                    wcopy(n + 1, i).start()
            for i in range(2):
                wcopy(n, i).wait()

            def mt(t, _):
                q = (n - G0) * tiles + t

                @pl.when(n == G0)
                def _():
                    ucopy(t).wait()

                @pl.when(q + 1 < NG * tiles)
                def _():
                    hcopy(q + 1).start()

                @pl.when(q >= 2)
                def _():
                    ycopy(q - 2).wait()
                hcopy(q).wait()
                rows = pl.ds(pl.multiple_of(t * MD, MD), MD)
                acc = None
                for a, b in KSPLIT:
                    part = jnp.dot(u[rows, a:b], wbuf[n % 2, a:b], preferred_element_type=F32)
                    acc = part if acc is None else acc + part
                yb[q % 2] = (hb[q % 2].astype(F32) + acc).astype(BF)
                ycopy(q).start()
                return 0
            lax.fori_loop(0, tiles, mt, 0)
            return 0
        lax.fori_loop(G0, N, step, 0)
        for q in (NG * tiles - 2, NG * tiles - 1):
            ycopy(jnp.int32(q)).wait()

    pl.run_scoped(down_phase, pltpu.VMEM((TOK, FFN), BF), pltpu.VMEM((2, FFN, FW), BF), pltpu.VMEM((2, MD, FW), BF), pltpu.VMEM((2, MD, FW), BF),
                  pltpu.SemaphoreType.DMA((TOK // MD,)), pltpu.SemaphoreType.DMA((2, 2)), pltpu.SemaphoreType.DMA((2,)), pltpu.SemaphoreType.DMA((2,)))


def local_layer(x_loc, norm_attn, w_query, w_key, w_value, w_out, norm_mlp, w_gate, w_up, w_down):
    shape = x_loc.shape
    x2 = x_loc.reshape(TOK, D)
    anys = pl.BlockSpec(memory_space=pl.ANY)
    vm = pl.BlockSpec(memory_space=pltpu.VMEM)

    def out(*sh):
        return jax.ShapeDtypeStruct(sh, BF)
    sem = pltpu.SemaphoreType.DMA
    res = pl.pallas_call(
        kernel,
        out_shape=[out(TOK, D), out(TOK, D), out(HD, D), out(HD, D), out(HD, D), out(HD, D), out(HD, FFN), out(HD, FFN), out(HF, D),
                   out(TOK, D), out(TOK, FFN), out(TOK, D)],
        in_specs=[anys, vm, vm] + [anys] * 7,
        out_specs=[anys] * 12,
        scratch_shapes=[pltpu.VMEM((2, HD // 128, 128), F32)] * 2 + [pltpu.VMEM((4, 1, HD), F32)]
        + [pltpu.VMEM((512, HEAD), F32)] * 2 + [pltpu.VMEM((512, 128), jnp.int32)] + [sem((NSEM,))] * 8 + [sem((2,)), sem((4, 3)), sem((4, 3)), sem((8, 3)), sem((8, 3))],
        compiler_params=pltpu.CompilerParams(collective_id=0, has_side_effects=True, vmem_limit_bytes=66_900_000),
        cost_estimate=pl.CostEstimate(flops=846 * 10**9, bytes_accessed=10**9, transcendentals=0),
        name='layer',
    )(x2, norm_attn.reshape(HD // 128, 128), norm_mlp.reshape(HD // 128, 128), w_query, w_key, w_value, w_out, w_gate, w_up, w_down)
    return res[0].reshape(shape)


def solution(mesh):
    rows = P(('dp', 'fsdp'), 'sp', None)
    weight = P('fsdp', None)
    gain = P('fsdp')
    specs = (rows, gain, weight, weight, weight, weight, gain, weight, weight, weight)
    return jax.shard_map(local_layer, mesh=mesh, in_specs=specs, out_specs=rows, check_vma=False)
```

```python
import math
import functools
import jax
import jax.numpy as jnp
from jax import lax
from jax.experimental import pallas as pl
from jax.experimental.pallas import tpu as pltpu
from jax.sharding import PartitionSpec as P

HEAD = 128
LN = HEAD
SEQ = 512
EPS = 1e-5
THETA = 5e7
NEG = -1e30
BF = jnp.bfloat16
F32 = jnp.float32
MESH = pl.DeviceIdType.MESH

D = 4096
HD = D // 2
FFN = 11008
HF = FFN // 2
TOK = 2048
GW = 256
CW = 512
FW = 256
ROWS = 8

NC, NE, NF, NG = 8, 8, 43, 16
E0 = NC
F0 = E0 + NE
G0 = F0 + NF
N = G0 + NG
YR, XR = 64, 32
FD = F0 + 3
F_E = 512
G_E = 1360
YAHEAD = 16
SLOTS = 2
KB = 1024
KSPLIT = ((0, 2816), (2816, 5632), (5632, 8448), (8448, FFN))
MT = 1024
NB = 64
MD = 512


def kernel(x_in, gattn, gmlp, wq, wk, wv, wo, wg, wu, wd,
           y, xr, rq, rk, rv, ro, rg, ru, rd, ob, ostage, psum, ubuf, hbuf,
           gown, grem, gains, cos, sin, qpos, ys, yr, xs, xrs, dys, dyr, dxs, dxr, gsem, xsend, xrecv, osend, orecv):
    f = lax.axis_index('fsdp')
    s = lax.axis_index('sp')
    cx = s // 2
    cc = s % 2
    ynbr = (0, 1 - f, s)
    xnbr = (0, f, (s + 2) % 4)
    pnbr = (0, f, cx * 2 + 1 - cc)

    def peer(k):
        if k == 1:
            return cx * 2 + 1 - cc
        if k == 2:
            return (s + 2) % 4
        return 3 - s

    bar = pltpu.get_barrier_semaphore()
    for dev in (ynbr, pnbr, xnbr, (0, f, 3 - s)):
        pl.semaphore_signal(bar, inc=1, device_id=dev, device_id_type=MESH)
    pl.semaphore_wait(bar, 4)

    def rcopy(src, dst, ssem, rsem, dev):
        return pltpu.make_async_remote_copy(src_ref=src, dst_ref=dst, send_sem=ssem, recv_sem=rsem, device_id=dev, device_id_type=MESH)

    class Part:
        def __init__(self, w, r, col, ncol, half, e, sem):
            self.w, self.r, self.half, self.e, self.m = w, r, half, e, half - 2 * e
            self.ysem, self.sem = sem % YR, sem % XR
            self.cols = pl.ds(col, ncol)

        def rows(self, off, n):
            return pl.ds(pl.multiple_of(cc * self.half + off, 16), n)

        def ycopy(self):
            a = (self.rows(cx * self.e, self.e + self.m), self.cols)
            return rcopy(self.w.at[a], self.r.at[a], ys.at[self.ysem], yr.at[self.ysem], ynbr)

        def xcopy(self):
            a = (self.rows(cx * (self.e + self.m), self.e), self.cols)
            return rcopy(self.r.at[a], self.r.at[a], xs.at[self.sem], xrs.at[self.sem], xnbr)

        def dycopy(self):
            a = (self.rows(cx * self.e, self.e + self.m), self.cols)
            return rcopy(self.r.at[a], self.r.at[a], dys.at[self.sem], dyr.at[self.sem], pnbr)

        def dxcopy(self):
            a = (self.rows((1 - cx) * (self.e + self.m), self.e), self.cols)
            return rcopy(self.r.at[a], self.r.at[a], dxs.at[self.sem], dxr.at[self.sem], pnbr)

        def ysend(self):
            self.ycopy().start()

        def yf(self):
            c = self.ycopy()
            c.wait_recv()
            if self.e:
                self.xcopy().start()
            self.dycopy().start()
            c.wait_send()

        def xf(self):
            if self.e:
                c = self.xcopy()
                c.wait_recv()
                self.dxcopy().start()
                c.wait_send()

        def done(self):
            c = self.dycopy()
            c.wait_recv()
            c.wait_send()
            if self.e:
                c = self.dxcopy()
                c.wait_recv()
                c.wait_send()

    def al(v, k):
        return v if isinstance(v, int) else pl.multiple_of(v, k)

    def when(cond, fn):
        if isinstance(cond, bool):
            if cond:
                fn()
        else:
            pl.when(cond)(fn)

    def item(n, what, cand):
        def run(pairs, col, ncol, half, e, sem):
            for i, (w, r) in enumerate(pairs):
                getattr(Part(w, r, col, ncol, half, e, sem + i), what)()

        if 'C' in cand:
            when(n < E0, lambda: run(((wq, rq), (wk, rk), (wv, rv)), pl.multiple_of(cx * HD + n * GW, GW), GW, HD // 2, 0, 3 * n))
        if 'E' in cand:
            when((n >= E0) & (n < F0), lambda: run(((wo, ro),), al((n - E0) * CW, CW), CW, HD // 2, 0, n + 2 * NC))
        if 'F' in cand:
            pairs = ((wg, rg), (wu, ru))
            if 'D' in cand:
                when((n >= F0) & (n < FD), lambda: run(pairs, al((n - F0) * FW, FW), FW, HD // 2, 0, 2 * n + 2 * NC - F0))
            when((n >= FD) & (n < G0), lambda: run(pairs, al((n - F0) * FW, FW), FW, HD // 2, F_E, 2 * n + 2 * NC - F0))
        if 'W' in cand or 'G' in cand:
            when((n >= G0) & (n < N - 1), lambda: run(((wd, rd),), al((n - G0) * FW, FW), FW, HF // 2, G_E, n + 2 * NC + NF))
        if 'G' in cand:
            when(n == N - 1, lambda: run(((wd, rd),), D - FW, FW, HF // 2, 0, n + 2 * NC + NF))

    gown[0] = gattn[...].astype(F32)
    gown[1] = gmlp[...].astype(F32)
    gcopy = rcopy(gown, grem, gsem.at[0], gsem.at[1], ynbr)
    gcopy.start()
    item(0, 'ysend', 'C')

    def xcopy(r, k):
        first = (cc if k == 2 else 1 - cc) * ROWS
        src = x_in.at[pl.ds(pl.multiple_of((first + r) * LN, LN), LN)]
        dst = xr.at[pl.ds(pl.multiple_of(r * SEQ + s * LN, LN), LN)]
        return rcopy(src, dst, xsend.at[r, k - 1], xrecv.at[r, k - 1], (0, f, peer(k)))

    for r in range(ROWS):
        for k in (2, 3, 1):
            xcopy(r, k).start()
    for n in range(1, 4):
        item(n, 'ysend', 'C')

    def positions(shape, dim):
        j = lax.broadcasted_iota(jnp.int32, shape, dim)
        return (j % LN) * 4 + j // LN

    def table(i, _):
        rs = pl.ds(pl.multiple_of(i * LN, LN), LN)
        pos = lax.broadcasted_iota(jnp.int32, (LN, HEAD), 0) * 4 + i
        lane = lax.broadcasted_iota(jnp.int32, (LN, HEAD), 1)
        freq = jnp.exp((lane % (HEAD // 2)).astype(F32) * (-2.0 * math.log(THETA) / HEAD))
        ang = pos.astype(F32) * freq
        qpos[rs, :] = pos
        cos[rs, :] = jnp.cos(ang)
        sn = jnp.sin(ang)
        sin[rs, :] = jnp.where(lane < HEAD // 2, -sn, sn)
        return 0
    lax.fori_loop(0, 4, table, 0)
    gcopy.wait_recv()
    gcopy.wait_send()
    for g in range(2):
        for i, src in enumerate((gown, grem)):
            v = src[g]
            gains[2 * g + i] = jnp.concatenate([v[k:k + 1] for k in range(HD // LN)], axis=1)

    def norm_tile(act, xt, t, row, g):
        def sub(i, _):
            for o in range(0, NB, 16):
                rs = pl.ds(pl.multiple_of(i * NB + o, 16), 16)
                x0 = xt[t, 0, rs, :].astype(F32)
                x1 = xt[t, 1, rs, :].astype(F32)
                ss = jnp.sum(x0 * x0, axis=-1, keepdims=True) + jnp.sum(x1 * x1, axis=-1, keepdims=True)
                inv = lax.rsqrt(ss * (1.0 / D) + EPS)
                to = pl.ds(pl.multiple_of(row + i * NB + o, 16), 16)
                act[0, to, :] = (xt[t, 0, rs, :].astype(F32) * inv * gains[2 * g]).astype(BF)
                act[1, to, :] = (xt[t, 1, rs, :].astype(F32) * inv * gains[2 * g + 1]).astype(BF)
            return 0
        lax.fori_loop(0, LN // NB, sub, 0)

    def halves(src, row, xt, t, sem):
        rows = pl.ds(row, LN)
        return [pltpu.make_async_copy(src.at[rows, pl.ds(pl.multiple_of(h * HD, HD), HD)], xt.at[t, i], sem.at[t, i])
                for i, h in enumerate((f, 1 - f))]

    def product(act, rows, wbuf, slot):
        acc = None
        for i in range(2):
            for k in range(0, HD, KB):
                part = jnp.dot(act[i, rows, k:k + KB], wbuf[slot, i, k:k + KB], preferred_element_type=F32)
                acc = part if acc is None else acc + part
        return acc

    def oremote(k):
        first = cc * ROWS * LN
        return rcopy(ostage.at[k - 1], ob.at[pl.ds(pl.multiple_of(first, LN), ROWS * LN), pl.ds(pl.multiple_of(cx * HD, HD), HD)],
                     osend.at[k - 1], orecv.at[k - 1], (0, f, peer(k)))

    def attention_phase(act, wbuf, obuf, xt, qb, kb, vb, wl, ol, xl):
        def wcopies(j, slot):
            cols = pl.ds(pl.multiple_of(cx * HD + j * GW, GW), GW)
            return [pltpu.make_async_copy(b.at[:, cols], wbuf.at[slot, i, :, pl.ds(t * GW, GW)], wl.at[slot, i, t])
                    for t, pair in enumerate(((wq, rq), (wk, rk), (wv, rv))) for i, b in enumerate(pair)]

        def tokens(r):
            for k in (1, 2, 3):
                c = xcopy(r, k)
                c.wait_recv()
                c.wait_send()

            def cps(t):
                return halves(xr, pl.multiple_of(r * SEQ + t * LN, LN), xt, t, xl)
            for t in range(4):
                @pl.when(s != t)
                def _():
                    for c in cps(t):
                        c.start()

                @pl.when(s == t)
                def _():
                    for c in halves(x_in, pl.multiple_of((cc * ROWS + r) * LN, LN), xt, t, xl):
                        c.start()
            for t in range(4):
                for c in cps(t):
                    c.wait()
                norm_tile(act, xt, t, r * SEQ + t * LN, 0)

        def rope(u):
            out = []
            for h in range(GW // HEAD):
                v = u[:, h * HEAD:(h + 1) * HEAD]
                out.append(v * cos[...] + pltpu.roll(v, HEAD // 2, 1) * sin[...])
            return jnp.concatenate(out, axis=1).astype(BF)

        def place(r, j):
            return (pl.ds(pl.multiple_of((cc * ROWS + r) * LN, LN), LN), pl.ds(pl.multiple_of(cx * HD + j * GW, GW), GW))

        def stage(r, j, k):
            return ostage.at[k - 1, pl.ds(pl.multiple_of(r * LN, LN), LN), pl.ds(pl.multiple_of(j * GW, GW), GW)]

        def ostore(r, j, slot):
            own = pltpu.make_async_copy(obuf.at[slot, pl.ds(pl.multiple_of(s * LN, LN), LN)], ob.at[place(r, j)], ol.at[slot, 0])
            return [own] + [pltpu.make_async_copy(obuf.at[slot, pl.ds(pl.multiple_of(peer(k) * LN, LN), LN)], stage(r, j, k), ol.at[slot, k])
                            for k in (1, 2, 3)]

        def osends(r, j, slot):
            for c in ostore(r, j, slot):
                c.wait()
            for k in (2, 3, 1):
                rcopy(stage(r, j, k), ob.at[place(r, j)], osend.at[k - 1], orecv.at[k - 1], (0, f, peer(k))).start()

        def shell(k, _):
            def unit(i, _):
                r = jnp.minimum(i, k)
                j = jnp.minimum(k, 2 * k - i)
                u = k * k + i
                slot = (k * (k + 1) // 2 + k - j) % 2

                def next_group():
                    item(k + 1, 'done', 'C')
                    for c in wcopies(k + 1, 1 - slot):
                        c.start()

                @pl.when(i == k)
                def _():
                    tokens(k)

                    @pl.when((k > 0) & (k < NC - 1))
                    def _():
                        item(k + 1, 'yf', 'C')

                @pl.when((i == 0) | (i > k))
                def _():
                    for c in wcopies(j, slot):
                        c.wait()

                    @pl.when(j > 0)
                    def _():
                        for c in wcopies(j - 1, 1 - slot):
                            c.start()

                    @pl.when((j == 0) & (k > 0) & (k < NC - 1))
                    def _():
                        next_group()

                rows = pl.ds(pl.multiple_of(r * SEQ, SEQ), SEQ)
                acc = product(act, rows, wbuf, slot)
                qb[...] = rope(acc[:, :GW])
                kb[...] = rope(acc[:, GW:2 * GW])
                vb[...] = acc[:, 2 * GW:].astype(BF)

                def head(h, _):
                    hs = pl.ds(pl.multiple_of(h * HEAD, HEAD), HEAD)
                    sc = lax.dot_general(qb[:, hs], kb[:, hs], (((1,), (1,)), ((), ())), preferred_element_type=F32)
                    qp = qpos[...]
                    kp = positions((1, SEQ), 1)
                    sc = jnp.where(jnp.concatenate([qp] * 4, axis=1) >= kp, sc, NEG)
                    mx = jnp.max(sc, axis=-1, keepdims=True)
                    p = jnp.exp2((sc - mx) * (HEAD ** -0.5 * math.log2(math.e)))
                    tot = jnp.sum(p, axis=-1, keepdims=True)
                    o = jnp.dot(p.astype(BF), vb[:, hs], preferred_element_type=F32) / tot
                    obuf[u % 2, :, hs] = o.astype(BF)
                    return 0
                lax.fori_loop(0, GW // HEAD, head, 0)
                for c in ostore(r, j, u % 2):
                    c.start()

                @pl.when(i > 0)
                def _():
                    osends(jnp.minimum(i - 1, k), jnp.minimum(k, 2 * k - i + 1), (u + 1) % 2)

                @pl.when((i == 0) & (k > 0))
                def _():
                    osends(k - 1, 0, (u + 1) % 2)

                @pl.when(u % 4 == 0)
                def _():
                    item(u // 4 + 4, 'ysend', 'CEFD')

                @pl.when(k == 0)
                def _():
                    item(1, 'yf', 'C')
                    next_group()
                return 0
            lax.fori_loop(0, 2 * k + 1, unit, 0)
            return 0

        item(0, 'yf', 'C')
        item(0, 'done', 'C')
        for c in wcopies(jnp.int32(0), jnp.int32(0)):
            c.start()
        lax.fori_loop(0, NC, shell, 0)
        osends(jnp.int32(ROWS - 1), jnp.int32(0), jnp.int32((NC * NC - 1) % 2))

    pl.run_scoped(attention_phase, pltpu.VMEM((2, ROWS * SEQ, HD), BF), pltpu.VMEM((2, 2, HD, 3 * GW), BF), pltpu.VMEM((2, SEQ, GW), BF),
                  pltpu.VMEM((4, 2, LN, HD), BF), pltpu.VMEM((SEQ, GW), BF), pltpu.VMEM((SEQ, GW), BF), pltpu.VMEM((SEQ, GW), BF),
                  pltpu.SemaphoreType.DMA((2, 2, 3)), pltpu.SemaphoreType.DMA((2, 4)), pltpu.SemaphoreType.DMA((4, 2)))

    for n in range(E0, F0):
        item(n, 'yf', 'E')
    for n in range(20, 24):
        item(n, 'ysend', 'FD')

    def dcopy(wdown, dl, n, i):
        cols = pl.ds(pl.multiple_of((n - G0) * FW, FW), FW)
        h = (f, 1 - f)[i]
        return pltpu.make_async_copy((wd, rd)[i].at[:, cols], wdown.at[n % 2, pl.ds(pl.multiple_of(h * HF, LN), HF)], dl.at[n % 2, i])

    def scope(wdown, dl, act, wbuf, obuf, wl, ol):
        def wcopies(n, cand):
            def go(fn):
                slot = n % SLOTS
                if 'F' in cand:
                    def ff():
                        cols = pl.ds(al((n - F0) * FW, FW), FW)
                        for i, pair in enumerate(((wg, wu), (rg, ru))):
                            for j, b in enumerate(pair):
                                fn(pltpu.make_async_copy(b.at[:, cols], wbuf.at[slot, i, :, pl.ds(j * FW, FW)], wl.at[slot, i + 2 * j]))
                    when((n >= F0) & (n < G0), ff)
            return go

        def load(n, cand):
            wcopies(n, cand)(lambda c: c.start())

        def loaded(n, cand):
            wcopies(n, cand)(lambda c: c.wait())

        def out_phase(hx, pb, hl, pp, al_):
            def ecopy(n, i):
                h = cx if i == 0 else 1 - cx
                cols = pl.ds(al((n - E0) * CW, CW), CW)
                return h, lambda w: pltpu.make_async_copy(w.at[:, cols], wbuf.at[n % SLOTS, i], wl.at[n % SLOTS, i])

            def eload(n, i):
                h, copy = ecopy(n, i)
                pl.when(h == f)(lambda: copy(wo).start())
                pl.when(h != f)(lambda: copy(ro).start())

            def eloaded(n, i):
                ecopy(n, i)[1](wo).wait()

            def acopy(t, i):
                h = cx if i == 0 else 1 - cx
                rows = pl.ds(t * MT, MT)
                return pltpu.make_async_copy(ob.at[rows, pl.ds(pl.multiple_of(h * HD, HD), HD)], act.at[i, rows], al_.at[t, i])

            def cols(n):
                return pl.ds(pl.multiple_of((n - E0) * CW, CW), CW)

            def xload(n):
                return pltpu.make_async_copy(x_in.at[:, cols(n)], hx.at[n % 2], hl.at[n % 2])

            def pstore(n):
                return pltpu.make_async_copy(pb.at[n % 2], psum.at[:, cols(n)], pp.at[0, n % 2])

            def pload(n):
                return pltpu.make_async_copy(psum.at[:, cols(n)], pb.at[n % 2], pp.at[1, n % 2])

            def hstore(n):
                return pltpu.make_async_copy(obuf.at[n % 2], hbuf.at[:, cols(n)], ol.at[n % 2])

            def eproduct(rows, slot, i):
                acc = None
                for k in range(0, HD, KB):
                    part = jnp.dot(act[i, rows, k:k + KB], wbuf[slot, i, k:k + KB], preferred_element_type=F32)
                    acc = part if acc is None else acc + part
                return acc

            first = jnp.int32(E0)
            item(E0, 'done', 'E')
            eload(first, 0)
            xload(first).start()
            c = oremote(1)
            c.wait_recv()
            c.wait_send()
            for t in range(TOK // MT):
                acopy(t, 0).start()
            for t in range(TOK // MT):
                acopy(t, 0).wait()

            def step1(n, _):
                @pl.when(n + 1 < F0)
                def _():
                    item(n + 1, 'done', 'E')
                    eload(n + 1, 0)
                    xload(n + 1).start()

                @pl.when(n >= E0 + 2)
                def _():
                    pstore(n - 2).wait()
                eloaded(n, 0)
                xload(n).wait()

                def mt(t, _):
                    rows = pl.ds(pl.multiple_of(t * MT, MT), MT)
                    pb[n % 2, rows, :] = hx[n % 2, rows, :].astype(F32) + eproduct(rows, n % SLOTS, 0)
                    return 0
                lax.fori_loop(0, TOK // MT, mt, 0)
                pstore(n).start()
                return 0
            lax.fori_loop(E0, F0, step1, 0)
            for n in (F0 - 2, F0 - 1):
                pstore(jnp.int32(n)).wait()
            eload(first, 1)
            pload(first).start()

            for n in range(F0, FD + 1):
                item(n, 'yf', 'FD')
            for k in (2, 3):
                c = oremote(k)
                c.wait_recv()
                c.wait_send()
            for t in range(TOK // MT):
                acopy(t, 1).start()
            for t in range(TOK // MT):
                acopy(t, 1).wait()

            def step2(n, _):
                item(n + YAHEAD, 'ysend', 'F')

                @pl.when((n == E0) | ((n - E0) * 2 // 5 > (n - E0 - 1) * 2 // 5))
                def _():
                    item(FD + 1 + (n - E0) * 2 // 5, 'yf', 'F')

                @pl.when(n + 1 < F0)
                def _():
                    eload(n + 1, 1)
                    pload(n + 1).start()

                @pl.when(n + 1 == F0)
                def _():
                    item(n + 1, 'done', 'FD')
                    load(n + 1, 'F')

                @pl.when(n >= E0 + 2)
                def _():
                    hstore(n - 2).wait()
                eloaded(n, 1)
                pload(n).wait()

                def mt(t, _):
                    rows = pl.ds(pl.multiple_of(t * MT, MT), MT)
                    obuf[n % 2, rows, :] = (pb[n % 2, rows, :] + eproduct(rows, n % SLOTS, 1)).astype(BF)
                    return 0
                lax.fori_loop(0, TOK // MT, mt, 0)
                hstore(n).start()
                return 0
            lax.fori_loop(E0, F0, step2, 0)
            for n in (F0 - 2, F0 - 1):
                hstore(jnp.int32(n)).wait()

        pl.run_scoped(out_phase, pltpu.VMEM((2, TOK, CW), BF), pltpu.VMEM((2, TOK, CW), F32), pltpu.SemaphoreType.DMA((2,)), pltpu.SemaphoreType.DMA((2, 2)),
                      pltpu.SemaphoreType.DMA((2, 2)))

        def norm_phase(xt, xl):
            def cps(i):
                return halves(hbuf, pl.multiple_of(i * LN, LN), xt, i % 4, xl)
            for i in range(3):
                for c in cps(jnp.int32(i)):
                    c.start()
            item(FD + 4, 'yf', 'F')

            def step(i, _):
                @pl.when(i + 3 < 16)
                def _():
                    for c in cps(i + 3):
                        c.start()
                for c in cps(i):
                    c.wait()
                norm_tile(act, xt, i % 4, i * LN, 1)
                return 0
            lax.fori_loop(0, 16, step, 0)

        pl.run_scoped(norm_phase, pltpu.VMEM((4, 2, LN, HD), BF), pltpu.SemaphoreType.DMA((4, 2)))

        def ustore(n):
            return pltpu.make_async_copy(obuf.at[n % 2, :, pl.ds(0, FW)], ubuf.at[:, pl.ds(pl.multiple_of((n - F0) * FW, FW), FW)], ol.at[n % 2])

        def gate_step(n, _):
            @pl.when(n >= F0 + 2)
            def _():
                ustore(n - 2).wait()
            loaded(n, 'F')
            slot = n % SLOTS

            def mt(t, _):
                @pl.when(t == 0)
                def _():
                    item(n + YAHEAD, 'ysend', 'FG')

                    @pl.when((n == F0) | ((n - F0) * 8 // 9 > (n - F0 - 1) * 8 // 9))
                    def _():
                        item(FD + 5 + (n - F0) * 8 // 9, 'yf', 'FG')
                    item(n + 1, 'xf', 'FG')

                @pl.when(t == 1)
                def _():
                    item(n + 1, 'done', 'FGD')
                    load(n + 1, 'F')

                    @pl.when(n + 1 == G0)
                    def _():
                        for i in range(2):
                            dcopy(wdown, dl, n + 1, i).start()
                rows = pl.ds(pl.multiple_of(t * MT, MT), MT)
                acc = product(act, rows, wbuf, slot)
                gate, up = acc[:, :FW], acc[:, FW:]
                obuf[n % 2, rows, pl.ds(0, FW)] = (gate * jax.nn.sigmoid(gate) * up).astype(BF)
                return 0
            lax.fori_loop(0, TOK // MT, mt, 0)
            ustore(n).start()
            return 0
        lax.fori_loop(F0, G0, gate_step, 0)
        for n in (G0 - 2, G0 - 1):
            ustore(jnp.int32(n)).wait()

    def down_phase(wdown, dl, u, hb, yb, ul, hl, yl):
        tiles = TOK // MD

        def ucopy(t):
            rows = pl.ds(pl.multiple_of(t * MD, MD), MD)
            return pltpu.make_async_copy(ubuf.at[rows], u.at[rows], ul.at[t])

        def at(q):
            return pl.ds(pl.multiple_of((q % tiles) * MD, MD), MD), pl.ds(pl.multiple_of((q // tiles) * FW, FW), FW)

        def hcopy(q):
            return pltpu.make_async_copy(hbuf.at[at(q)], hb.at[q % 2], hl.at[q % 2])

        def ycopy(q):
            return pltpu.make_async_copy(yb.at[q % 2], y.at[at(q)], yl.at[q % 2])

        hcopy(jnp.int32(0)).start()
        for t in range(tiles):
            ucopy(t).start()

        def tile(n, t, loading):
            q = (n - G0) * tiles + t

            if loading:
                @pl.when(t % 2 == 0)
                def _():
                    item(G0 + 3 + t // 2, 'yf', 'G')
            else:
                p = q - tiles

                @pl.when((p == 0) | (4 * p // 19 > 4 * (p - 1) // 19))
                def _():
                    item(G0 + 5 + 4 * p // 19, 'yf', 'W')

            @pl.when((t == 1) & (n == N - 2))
            def _():
                item(N - 1, 'yf', 'G')

            @pl.when(t == 1)
            def _():
                item(n + 1, 'xf', 'G')

            @pl.when((t == tiles - 1) & (n + 1 < N))
            def _():
                item(n + 1, 'done', 'G')
                for i in range(2):
                    dcopy(wdown, dl, n + 1, i).start()

            @pl.when(q + 1 < NG * tiles)
            def _():
                hcopy(q + 1).start()

            @pl.when(q >= 2)
            def _():
                ycopy(q - 2).wait()
            hcopy(q).wait()
            rows = pl.ds(pl.multiple_of(t * MD, MD), MD)
            acc = None
            if loading:
                ucopy(t).wait()
            for a, b in KSPLIT:
                part = jnp.dot(u[rows, a:b], wdown[n % 2, a:b], preferred_element_type=F32)
                acc = part if acc is None else acc + part
            yb[q % 2] = (hb[q % 2].astype(F32) + acc).astype(BF)
            ycopy(q).start()

        def step(n, loading):
            for i in range(2):
                dcopy(wdown, dl, n, i).wait()

            def mt(t, _):
                tile(n, t, loading)
                return 0
            lax.fori_loop(0, tiles, mt, 0)
            return 0

        step(jnp.int32(G0), True)
        lax.fori_loop(G0 + 1, N, lambda n, _: step(n, False), 0)
        for q in (NG * tiles - 2, NG * tiles - 1):
            ycopy(jnp.int32(q)).wait()

    def last_scope(wdown, dl):
        dma = pltpu.SemaphoreType.DMA
        pl.run_scoped(functools.partial(scope, wdown, dl), pltpu.VMEM((2, TOK, HD), BF), pltpu.VMEM((SLOTS, 2, HD, CW), BF), pltpu.VMEM((2, TOK, CW), BF),
                      dma((SLOTS, 4)), dma((2,)))
        pl.run_scoped(functools.partial(down_phase, wdown, dl), pltpu.VMEM((TOK, FFN), BF), pltpu.VMEM((2, MD, FW), BF), pltpu.VMEM((2, MD, FW), BF),
                      dma((TOK // MD,)), dma((2,)), dma((2,)))

    pl.run_scoped(last_scope, pltpu.VMEM((2, FFN, FW), BF), pltpu.SemaphoreType.DMA((2, 2)))


def local_layer(x_loc, norm_attn, w_query, w_key, w_value, w_out, norm_mlp, w_gate, w_up, w_down):
    shape = x_loc.shape
    x2 = x_loc.reshape(TOK, D)
    anys = pl.BlockSpec(memory_space=pl.ANY)
    vm = pl.BlockSpec(memory_space=pltpu.VMEM)

    def out(*sh):
        return jax.ShapeDtypeStruct(sh, BF)
    sem = pltpu.SemaphoreType.DMA
    res = pl.pallas_call(
        kernel,
        out_shape=[out(TOK, D), out(ROWS * SEQ, D), out(HD, D), out(HD, D), out(HD, D), out(HD, D), out(HD, FFN), out(HD, FFN), out(HF, D),
                   out(TOK, D), out(3, ROWS * LN, HD), jax.ShapeDtypeStruct((TOK, D), F32), out(TOK, FFN), out(TOK, D)],
        in_specs=[anys, vm, vm] + [anys] * 7,
        out_specs=[anys] * 14,
        scratch_shapes=[pltpu.VMEM((2, HD // LN, LN), F32)] * 2 + [pltpu.VMEM((4, 1, HD), F32)]
        + [pltpu.VMEM((SEQ, HEAD), F32)] * 2 + [pltpu.VMEM((SEQ, LN), jnp.int32)] + [sem((YR,))] * 2 + [sem((XR,))] * 6 + [sem((2,)), sem((ROWS, 3)), sem((ROWS, 3)), sem((3,)), sem((3,))],
        compiler_params=pltpu.CompilerParams(collective_id=0, has_side_effects=True, vmem_limit_bytes=66_900_000),
        cost_estimate=pl.CostEstimate(flops=846 * 10**9, bytes_accessed=10**9, transcendentals=0),
        name='layer',
    )(x2, norm_attn.reshape(HD // LN, LN), norm_mlp.reshape(HD // LN, LN), w_query, w_key, w_value, w_out, w_gate, w_up, w_down)
    return res[0].reshape(shape)


def solution(mesh):
    rows = P(('dp', 'fsdp'), 'sp', None)
    weight = P('fsdp', None)
    gain = P('fsdp')
    specs = (rows, gain, weight, weight, weight, weight, gain, weight, weight, weight)
    return jax.shard_map(local_layer, mesh=mesh, in_specs=specs, out_specs=rows, check_vma=False)
```

```python
import math
import functools
import jax
import jax.numpy as jnp
from jax import lax
from jax.experimental import pallas as pl
from jax.experimental.pallas import tpu as pltpu
from jax.sharding import PartitionSpec as P

HEAD = 128
LN = HEAD
SEQ = 512
EPS = 1e-5
THETA = 5e7
NEG = -1e30
BF = jnp.bfloat16
F32 = jnp.float32
MESH = pl.DeviceIdType.MESH

D = 4096
HD = D // 2
FFN = 11008
HF = FFN // 2
TOK = 2048
GW = 256
CW = 512
FW = 256
ROWS = 8

NC, NE, NF, NG = 8, 8, 43, 16
E0 = NC
F0 = E0 + NE
G0 = F0 + NF
N = G0 + NG
YR, XR = 64, 32
FD = F0 + 3
F_E = 512
G_E = 1360
G_L = 352
YAHEAD = 16
SLOTS = 2
KB = 1024
KSPLIT = tuple(range(0, FFN - 1792, 1792)) + (FFN,)
OWNK = 3, 1792
RESTK = 2, 2816
MT = 1024
NB = 64
MD = 512


def kernel(x_in, gattn, gmlp, wq, wk, wv, wo, wg, wu, wd,
           y, xr, rq, rk, rv, ro, rg, ru, rd, ob, ostage, psum, ubuf, hbuf,
           gown, grem, gains, ys, yr, xs, xrs, dys, dyr, dxs, dxr, gsem, xsend, xrecv, osend, orecv):
    f = lax.axis_index('fsdp')
    s = lax.axis_index('sp')
    cx = s // 2
    cc = s % 2
    ynbr = (0, 1 - f, s)
    xnbr = (0, f, (s + 2) % 4)
    pnbr = (0, f, cx * 2 + 1 - cc)

    def peer(k):
        if k == 1:
            return cx * 2 + 1 - cc
        if k == 2:
            return (s + 2) % 4
        return 3 - s

    bar = pltpu.get_barrier_semaphore()
    for dev in (ynbr, pnbr, xnbr, (0, f, 3 - s)):
        pl.semaphore_signal(bar, inc=1, device_id=dev, device_id_type=MESH)
    pl.semaphore_wait(bar, 4)

    def rcopy(src, dst, ssem, rsem, dev):
        return pltpu.make_async_remote_copy(src_ref=src, dst_ref=dst, send_sem=ssem, recv_sem=rsem, device_id=dev, device_id_type=MESH)

    class Part:
        def __init__(self, w, r, col, ncol, half, e, sem):
            self.w, self.r, self.half, self.e, self.m = w, r, half, e, half - 2 * e
            self.ysem, self.sem = sem % YR, sem % XR
            self.cols = pl.ds(col, ncol)

        def rows(self, off, n):
            return pl.ds(pl.multiple_of(cc * self.half + off, 16), n)

        def ycopy(self):
            a = (self.rows(cx * self.e, self.e + self.m), self.cols)
            return rcopy(self.w.at[a], self.r.at[a], ys.at[self.ysem], yr.at[self.ysem], ynbr)

        def xcopy(self):
            a = (self.rows(cx * (self.e + self.m), self.e), self.cols)
            return rcopy(self.r.at[a], self.r.at[a], xs.at[self.sem], xrs.at[self.sem], xnbr)

        def dycopy(self):
            a = (self.rows(cx * self.e, self.e + self.m), self.cols)
            return rcopy(self.r.at[a], self.r.at[a], dys.at[self.sem], dyr.at[self.sem], pnbr)

        def dxcopy(self):
            a = (self.rows((1 - cx) * (self.e + self.m), self.e), self.cols)
            return rcopy(self.r.at[a], self.r.at[a], dxs.at[self.sem], dxr.at[self.sem], pnbr)

        def ysend(self):
            self.ycopy().start()

        def yf(self):
            c = self.ycopy()
            c.wait_recv()
            if self.e:
                self.xcopy().start()
            self.dycopy().start()
            c.wait_send()

        def xf(self):
            if self.e:
                c = self.xcopy()
                c.wait_recv()
                self.dxcopy().start()
                c.wait_send()

        def done(self):
            c = self.dycopy()
            c.wait_recv()
            c.wait_send()
            if self.e:
                c = self.dxcopy()
                c.wait_recv()
                c.wait_send()

    def al(v, k):
        return v if isinstance(v, int) else pl.multiple_of(v, k)

    def when(cond, fn):
        if isinstance(cond, bool):
            if cond:
                fn()
        else:
            pl.when(cond)(fn)

    def item(n, what, cand):
        def run(pairs, col, ncol, half, e, sem):
            for i, (w, r) in enumerate(pairs):
                getattr(Part(w, r, col, ncol, half, e, sem + i), what)()

        if 'C' in cand:
            when(n < E0, lambda: run(((wq, rq), (wk, rk), (wv, rv)), pl.multiple_of(cx * HD + n * GW, GW), GW, HD // 2, 0, 3 * n))
        if 'E' in cand:
            when((n >= E0) & (n < F0), lambda: run(((wo, ro),), al((n - E0) * CW, CW), CW, HD // 2, 0, n + 2 * NC))
        if 'F' in cand:
            pairs = ((wg, rg), (wu, ru))
            if 'D' in cand:
                when((n >= F0) & (n < FD), lambda: run(pairs, al((n - F0) * FW, FW), FW, HD // 2, 0, 2 * n + 2 * NC - F0))
            when((n >= FD) & (n < G0), lambda: run(pairs, al((n - F0) * FW, FW), FW, HD // 2, F_E, 2 * n + 2 * NC - F0))
        if 'W' in cand or 'G' in cand:
            when((n >= G0) & (n < N - 1), lambda: run(((wd, rd),), al((n - G0) * FW, FW), FW, HF // 2, G_E, n + 2 * NC + NF))
        if 'G' in cand:
            when(n == N - 1, lambda: run(((wd, rd),), D - FW, FW, HF // 2, G_L, n + 2 * NC + NF))

    gown[0] = gattn[...].astype(F32)
    gown[1] = gmlp[...].astype(F32)
    gcopy = rcopy(gown, grem, gsem.at[0], gsem.at[1], ynbr)
    gcopy.start()
    item(0, 'ysend', 'C')

    def xcopy(r, k):
        first = (cc if k == 2 else 1 - cc) * ROWS
        src = x_in.at[pl.ds(pl.multiple_of((first + r) * LN, LN), LN)]
        dst = xr.at[pl.ds(pl.multiple_of(r * SEQ + s * LN, LN), LN)]
        return rcopy(src, dst, xsend.at[r, k - 1], xrecv.at[r, k - 1], (0, f, peer(k)))

    for r in range(ROWS):
        for k in (2, 3, 1):
            xcopy(r, k).start()
    for n in range(1, 4):
        item(n, 'ysend', 'C')

    def positions(shape, dim):
        j = lax.broadcasted_iota(jnp.int32, shape, dim)
        return (j % LN) * 4 + j // LN

    gcopy.wait_recv()
    gcopy.wait_send()
    for g in range(2):
        for i, src in enumerate((gown, grem)):
            v = src[g]
            gains[2 * g + i] = jnp.concatenate([v[k:k + 1] for k in range(HD // LN)], axis=1)

    def norm_tile(act, xt, t, row, g):
        def sub(i, _):
            for o in range(0, NB, 16):
                rs = pl.ds(pl.multiple_of(i * NB + o, 16), 16)
                x0 = xt[t, 0, rs, :].astype(F32)
                x1 = xt[t, 1, rs, :].astype(F32)
                ss = jnp.sum(x0 * x0, axis=-1, keepdims=True) + jnp.sum(x1 * x1, axis=-1, keepdims=True)
                inv = lax.rsqrt(ss * (1.0 / D) + EPS)
                to = pl.ds(pl.multiple_of(row + i * NB + o, 16), 16)
                act[0, to, :] = (xt[t, 0, rs, :].astype(F32) * inv * gains[2 * g]).astype(BF)
                act[1, to, :] = (xt[t, 1, rs, :].astype(F32) * inv * gains[2 * g + 1]).astype(BF)
            return 0
        lax.fori_loop(0, LN // NB, sub, 0)

    def halves(src, row, xt, t, sem):
        rows = pl.ds(row, LN)
        return [pltpu.make_async_copy(src.at[rows, pl.ds(pl.multiple_of(h * HD, HD), HD)], xt.at[t, i], sem.at[t, i])
                for i, h in enumerate((f, 1 - f))]

    def product(act, rows, wbuf, slot):
        acc = None
        for i in range(2):
            for k in range(0, HD, KB):
                part = jnp.dot(act[i, rows, k:k + KB], wbuf[slot, i, k:k + KB], preferred_element_type=F32)
                acc = part if acc is None else acc + part
        return acc

    def oremote(k):
        first = cc * ROWS * LN
        return rcopy(ostage.at[k - 1], ob.at[pl.ds(pl.multiple_of(first, LN), ROWS * LN), pl.ds(pl.multiple_of(cx * HD, HD), HD)],
                     osend.at[k - 1], orecv.at[k - 1], (0, f, peer(k)))

    def attention_phase(cos, sin, qpos, act, wbuf, obuf, xt, qb, kb, vb, wl, ol, xl):
        def table(i, _):
            rs = pl.ds(pl.multiple_of(i * LN, LN), LN)
            pos = lax.broadcasted_iota(jnp.int32, (LN, HEAD), 0) * 4 + i
            lane = lax.broadcasted_iota(jnp.int32, (LN, HEAD), 1)
            freq = jnp.exp((lane % (HEAD // 2)).astype(F32) * (-2.0 * math.log(THETA) / HEAD))
            ang = pos.astype(F32) * freq
            qpos[rs, :] = pos
            cos[rs, :] = jnp.cos(ang)
            sn = jnp.sin(ang)
            sin[rs, :] = jnp.where(lane < HEAD // 2, -sn, sn)
            return 0
        lax.fori_loop(0, 4, table, 0)

        def wcopies(j, slot):
            cols = pl.ds(pl.multiple_of(cx * HD + j * GW, GW), GW)
            return [pltpu.make_async_copy(b.at[:, cols], wbuf.at[slot, i, :, pl.ds(t * GW, GW)], wl.at[slot, i, t])
                    for t, pair in enumerate(((wq, rq), (wk, rk), (wv, rv))) for i, b in enumerate(pair)]

        def tokens(r):
            for k in (1, 2, 3):
                c = xcopy(r, k)
                c.wait_recv()
                c.wait_send()

            def cps(t):
                return halves(xr, pl.multiple_of(r * SEQ + t * LN, LN), xt, t, xl)
            for t in range(4):
                @pl.when(s != t)
                def _():
                    for c in cps(t):
                        c.start()

                @pl.when(s == t)
                def _():
                    for c in halves(x_in, pl.multiple_of((cc * ROWS + r) * LN, LN), xt, t, xl):
                        c.start()
            for t in range(4):
                for c in cps(t):
                    c.wait()
                norm_tile(act, xt, t, r * SEQ + t * LN, 0)

        def rope(u):
            out = []
            for h in range(GW // HEAD):
                v = u[:, h * HEAD:(h + 1) * HEAD]
                out.append(v * cos[...] + pltpu.roll(v, HEAD // 2, 1) * sin[...])
            return jnp.concatenate(out, axis=1).astype(BF)

        def place(r, j):
            return (pl.ds(pl.multiple_of((cc * ROWS + r) * LN, LN), LN), pl.ds(pl.multiple_of(cx * HD + j * GW, GW), GW))

        def stage(r, j, k):
            return ostage.at[k - 1, pl.ds(pl.multiple_of(r * LN, LN), LN), pl.ds(pl.multiple_of(j * GW, GW), GW)]

        def ostore(r, j, slot):
            own = pltpu.make_async_copy(obuf.at[slot, pl.ds(pl.multiple_of(s * LN, LN), LN)], ob.at[place(r, j)], ol.at[slot, 0])
            return [own] + [pltpu.make_async_copy(obuf.at[slot, pl.ds(pl.multiple_of(peer(k) * LN, LN), LN)], stage(r, j, k), ol.at[slot, k])
                            for k in (1, 2, 3)]

        def osends(r, j, slot):
            for c in ostore(r, j, slot):
                c.wait()
            for k in (2, 3, 1):
                rcopy(stage(r, j, k), ob.at[place(r, j)], osend.at[k - 1], orecv.at[k - 1], (0, f, peer(k))).start()

        def shell(k, _):
            def unit(i, _):
                r = jnp.minimum(i, k)
                j = jnp.minimum(k, 2 * k - i)
                u = k * k + i
                slot = (k * (k + 1) // 2 + k - j) % 2

                def next_group():
                    item(k + 1, 'done', 'C')
                    for c in wcopies(k + 1, 1 - slot):
                        c.start()

                @pl.when(i == k)
                def _():
                    tokens(k)

                    @pl.when((k > 0) & (k < NC - 1))
                    def _():
                        item(k + 1, 'yf', 'C')

                @pl.when((i == 0) | (i > k))
                def _():
                    for c in wcopies(j, slot):
                        c.wait()

                    @pl.when(j > 0)
                    def _():
                        for c in wcopies(j - 1, 1 - slot):
                            c.start()

                    @pl.when((j == 0) & (k > 0) & (k < NC - 1))
                    def _():
                        next_group()

                rows = pl.ds(pl.multiple_of(r * SEQ, SEQ), SEQ)
                acc = product(act, rows, wbuf, slot)
                qb[...] = rope(acc[:, :GW])
                kb[...] = rope(acc[:, GW:2 * GW])
                vb[...] = acc[:, 2 * GW:].astype(BF)

                def head(h, _):
                    hs = pl.ds(pl.multiple_of(h * HEAD, HEAD), HEAD)
                    sc = lax.dot_general(qb[:, hs], kb[:, hs], (((1,), (1,)), ((), ())), preferred_element_type=F32)
                    qp = qpos[...]
                    kp = positions((1, SEQ), 1)
                    sc = jnp.where(jnp.concatenate([qp] * 4, axis=1) >= kp, sc, NEG)
                    mx = jnp.max(sc, axis=-1, keepdims=True)
                    p = jnp.exp2((sc - mx) * (HEAD ** -0.5 * math.log2(math.e)))
                    tot = jnp.sum(p, axis=-1, keepdims=True)
                    o = jnp.dot(p.astype(BF), vb[:, hs], preferred_element_type=F32) / tot
                    obuf[u % 2, :, hs] = o.astype(BF)
                    return 0
                lax.fori_loop(0, GW // HEAD, head, 0)
                for c in ostore(r, j, u % 2):
                    c.start()

                @pl.when(i > 0)
                def _():
                    osends(jnp.minimum(i - 1, k), jnp.minimum(k, 2 * k - i + 1), (u + 1) % 2)

                @pl.when((i == 0) & (k > 0))
                def _():
                    osends(k - 1, 0, (u + 1) % 2)

                @pl.when(u % 4 == 0)
                def _():
                    item(u // 4 + 4, 'ysend', 'CEFD')

                @pl.when(k == 0)
                def _():
                    item(1, 'yf', 'C')
                    next_group()
                return 0
            lax.fori_loop(0, 2 * k + 1, unit, 0)
            return 0

        item(0, 'yf', 'C')
        item(0, 'done', 'C')
        for c in wcopies(jnp.int32(0), jnp.int32(0)):
            c.start()
        lax.fori_loop(0, NC, shell, 0)
        osends(jnp.int32(ROWS - 1), jnp.int32(0), jnp.int32((NC * NC - 1) % 2))

    pl.run_scoped(attention_phase, pltpu.VMEM((SEQ, HEAD), F32), pltpu.VMEM((SEQ, HEAD), F32), pltpu.VMEM((SEQ, LN), jnp.int32), pltpu.VMEM((2, ROWS * SEQ, HD), BF), pltpu.VMEM((2, 2, HD, 3 * GW), BF), pltpu.VMEM((2, SEQ, GW), BF),
                  pltpu.VMEM((4, 2, LN, HD), BF), pltpu.VMEM((SEQ, GW), BF), pltpu.VMEM((SEQ, GW), BF), pltpu.VMEM((SEQ, GW), BF),
                  pltpu.SemaphoreType.DMA((2, 2, 3)), pltpu.SemaphoreType.DMA((2, 4)), pltpu.SemaphoreType.DMA((4, 2)))

    for n in range(E0, F0):
        item(n, 'yf', 'E')
    for n in range(20, 24):
        item(n, 'ysend', 'FD')

    def dcopy(wdown, dl, n, i):
        cols = pl.ds(pl.multiple_of((n - G0) * FW, FW), FW)
        h = (f, 1 - f)[i]
        return pltpu.make_async_copy((wd, rd)[i].at[:, cols], wdown.at[n % 2, pl.ds(pl.multiple_of(h * HF, LN), HF)], dl.at[n % 2, i])

    def ahead(wdown, dl, i):
        slot = (G0 + 1) % 2
        return pltpu.make_async_copy(wd.at[:, pl.ds(D - (2 - i) * FW, FW)], wdown.at[slot, pl.ds(i * HF, HF)], dl.at[slot, i])

    def scope(wdown, dl, act, wbuf, obuf, wl, ol):
        def wcopies(n, cand):
            def go(fn):
                slot = n % SLOTS
                if 'F' in cand:
                    def ff():
                        cols = pl.ds(al((n - F0) * FW, FW), FW)
                        for i, pair in enumerate(((wg, wu), (rg, ru))):
                            for j, b in enumerate(pair):
                                fn(pltpu.make_async_copy(b.at[:, cols], wbuf.at[slot, i, :, pl.ds(j * FW, FW)], wl.at[slot, i + 2 * j]))
                    when((n >= F0) & (n < G0), ff)
            return go

        def load(n, cand):
            wcopies(n, cand)(lambda c: c.start())

        def loaded(n, cand):
            wcopies(n, cand)(lambda c: c.wait())

        def out_phase(hx, pb, hl, pp, al_):
            def ecopy(n, i):
                h = cx if i == 0 else 1 - cx
                cols = pl.ds(al((n - E0) * CW, CW), CW)
                return h, lambda w: pltpu.make_async_copy(w.at[:, cols], wbuf.at[n % SLOTS, i], wl.at[n % SLOTS, i])

            def eload(n, i):
                h, copy = ecopy(n, i)
                pl.when(h == f)(lambda: copy(wo).start())
                pl.when(h != f)(lambda: copy(ro).start())

            def eloaded(n, i):
                ecopy(n, i)[1](wo).wait()

            def acopy(t, i):
                h = cx if i == 0 else 1 - cx
                rows = pl.ds(t * MT, MT)
                return pltpu.make_async_copy(ob.at[rows, pl.ds(pl.multiple_of(h * HD, HD), HD)], act.at[i, rows], al_.at[t, i])

            def cols(n):
                return pl.ds(pl.multiple_of((n - E0) * CW, CW), CW)

            def xload(n):
                return pltpu.make_async_copy(x_in.at[:, cols(n)], hx.at[n % 2], hl.at[n % 2])

            def pstore(n):
                return pltpu.make_async_copy(pb.at[n % 2], psum.at[:, cols(n)], pp.at[0, n % 2])

            def pload(n):
                return pltpu.make_async_copy(psum.at[:, cols(n)], pb.at[n % 2], pp.at[1, n % 2])

            def hstore(n):
                return pltpu.make_async_copy(obuf.at[n % 2], hbuf.at[:, cols(n)], ol.at[n % 2])

            def eproduct(rows, slot, i):
                acc = None
                for k in range(0, HD, KB):
                    part = jnp.dot(act[i, rows, k:k + KB], wbuf[slot, i, k:k + KB], preferred_element_type=F32)
                    acc = part if acc is None else acc + part
                return acc

            first = jnp.int32(E0)
            item(E0, 'done', 'E')
            eload(first, 0)
            xload(first).start()
            c = oremote(1)
            c.wait_recv()
            c.wait_send()
            for t in range(TOK // MT):
                acopy(t, 0).start()
            for t in range(TOK // MT):
                acopy(t, 0).wait()

            def step1(n, _):
                @pl.when(n + 1 < F0)
                def _():
                    item(n + 1, 'done', 'E')
                    eload(n + 1, 0)
                    xload(n + 1).start()

                @pl.when(n >= E0 + 2)
                def _():
                    pstore(n - 2).wait()
                eloaded(n, 0)
                xload(n).wait()

                def mt(t, _):
                    rows = pl.ds(pl.multiple_of(t * MT, MT), MT)
                    pb[n % 2, rows, :] = hx[n % 2, rows, :].astype(F32) + eproduct(rows, n % SLOTS, 0)
                    return 0
                lax.fori_loop(0, TOK // MT, mt, 0)
                pstore(n).start()
                return 0
            lax.fori_loop(E0, F0, step1, 0)
            for n in (F0 - 2, F0 - 1):
                pstore(jnp.int32(n)).wait()
            eload(first, 1)
            pload(first).start()

            for n in range(F0, FD + 1):
                item(n, 'yf', 'FD')
            for k in (2, 3):
                c = oremote(k)
                c.wait_recv()
                c.wait_send()
            for t in range(TOK // MT):
                acopy(t, 1).start()
            for t in range(TOK // MT):
                acopy(t, 1).wait()

            def step2(n, _):
                item(n + YAHEAD, 'ysend', 'F')

                @pl.when((n == E0) | ((n - E0) * 2 // 5 > (n - E0 - 1) * 2 // 5))
                def _():
                    item(FD + 1 + (n - E0) * 2 // 5, 'yf', 'F')

                @pl.when(n + 1 < F0)
                def _():
                    eload(n + 1, 1)
                    pload(n + 1).start()

                @pl.when(n + 1 == F0)
                def _():
                    item(n + 1, 'done', 'FD')
                    load(n + 1, 'F')

                @pl.when(n >= E0 + 2)
                def _():
                    hstore(n - 2).wait()
                eloaded(n, 1)
                pload(n).wait()

                def mt(t, _):
                    rows = pl.ds(pl.multiple_of(t * MT, MT), MT)
                    obuf[n % 2, rows, :] = (pb[n % 2, rows, :] + eproduct(rows, n % SLOTS, 1)).astype(BF)
                    return 0
                lax.fori_loop(0, TOK // MT, mt, 0)
                hstore(n).start()
                return 0
            lax.fori_loop(E0, F0, step2, 0)
            for n in (F0 - 2, F0 - 1):
                hstore(jnp.int32(n)).wait()

        pl.run_scoped(out_phase, pltpu.VMEM((2, TOK, CW), BF), pltpu.VMEM((2, TOK, CW), F32), pltpu.SemaphoreType.DMA((2,)), pltpu.SemaphoreType.DMA((2, 2)),
                      pltpu.SemaphoreType.DMA((2, 2)))

        def norm_phase(xt, xl):
            def cps(i):
                return halves(hbuf, pl.multiple_of(i * LN, LN), xt, i % 4, xl)
            for i in range(3):
                for c in cps(jnp.int32(i)):
                    c.start()
            item(FD + 4, 'yf', 'F')

            def step(i, _):
                @pl.when(i + 3 < 16)
                def _():
                    for c in cps(i + 3):
                        c.start()
                for c in cps(i):
                    c.wait()
                norm_tile(act, xt, i % 4, i * LN, 1)
                return 0
            lax.fori_loop(0, 16, step, 0)

        pl.run_scoped(norm_phase, pltpu.VMEM((4, 2, LN, HD), BF), pltpu.SemaphoreType.DMA((4, 2)))

        def ustore(n):
            return pltpu.make_async_copy(obuf.at[n % 2, :, pl.ds(0, FW)], ubuf.at[:, pl.ds(pl.multiple_of((n - F0) * FW, FW), FW)], ol.at[n % 2])

        def gate_step(n, _):
            @pl.when(n >= F0 + 2)
            def _():
                ustore(n - 2).wait()
            loaded(n, 'F')
            slot = n % SLOTS

            def mt(t, _):
                @pl.when(t == 0)
                def _():
                    item(n + YAHEAD, 'ysend', 'FG')

                    @pl.when((n == F0) | ((n - F0) * 8 // 9 > (n - F0 - 1) * 8 // 9))
                    def _():
                        item(FD + 5 + (n - F0) * 8 // 9, 'yf', 'FG')
                    item(n + 1, 'xf', 'FG')

                @pl.when(t == 1)
                def _():
                    item(n + 1, 'done', 'FGD')
                    load(n + 1, 'F')

                    @pl.when(n + 1 == G0)
                    def _():
                        for i in range(2):
                            dcopy(wdown, dl, n + 1, i).start()
                            ahead(wdown, dl, i).start()
                rows = pl.ds(pl.multiple_of(t * MT, MT), MT)
                acc = product(act, rows, wbuf, slot)
                gate, up = acc[:, :FW], acc[:, FW:]
                obuf[n % 2, rows, pl.ds(0, FW)] = (gate * jax.nn.sigmoid(gate) * up).astype(BF)
                return 0
            lax.fori_loop(0, TOK // MT, mt, 0)
            ustore(n).start()
            return 0
        lax.fori_loop(F0, G0, gate_step, 0)
        for n in (G0 - 2, G0 - 1):
            ustore(jnp.int32(n)).wait()

    def down_phase(wdown, dl, u, hb, yb, sb, ul, hl, yl, sl):
        tiles = TOK // MD

        def ucopy(t):
            rows = pl.ds(pl.multiple_of(t * MD, MD), MD)
            return pltpu.make_async_copy(ubuf.at[rows], u.at[rows], ul.at[t])

        def at(q):
            return pl.ds(pl.multiple_of((q % tiles) * MD, MD), MD), pl.ds(pl.multiple_of((q // tiles) * FW, FW), FW)

        def hcopy(q):
            return pltpu.make_async_copy(hbuf.at[at(q)], hb.at[q % 2], hl.at[q % 2])

        def ycopy(q):
            return pltpu.make_async_copy(yb.at[q % 2], y.at[at(q)], yl.at[q % 2])

        hcopy(jnp.int32(0)).start()
        for t in range(tiles):
            ucopy(t).start()

        def tail_copy(t, i):
            rows = pl.ds(pl.multiple_of(t * MD, MD), MD)
            return psum.at[rows, pl.ds(pl.multiple_of(D + (i - 2) * FW, FW), FW)]

        def tail_store(t, i):
            return pltpu.make_async_copy(sb.at[i], tail_copy(t, i), sl.at[i])

        def tail_load(q):
            return pltpu.make_async_copy(tail_copy(q % tiles, q // tiles - (NG - 2)), sb.at[q % 2], sl.at[q % 2])

        def dots(t, slot):
            rows = pl.ds(pl.multiple_of(t * MD, MD), MD)
            acc = None
            for a, b in zip(KSPLIT, KSPLIT[1:]):
                part = jnp.dot(u[rows, a:b], wdown[slot, a:b], preferred_element_type=F32)
                acc = part if acc is None else acc + part
            return acc

        def add_dots(i, t, ustart, wstart, slot, pieces):
            count, k = pieces
            rows = pl.ds(pl.multiple_of(t * MD, MD), MD)

            def piece(j, _):
                us = pl.ds(pl.multiple_of(ustart + j * k, 2 * LN), k)
                ws = pl.ds(pl.multiple_of(wstart + j * k, LN), k)
                sb[i] += jnp.dot(u[rows, us], wdown[slot, ws], preferred_element_type=F32)
                return 0
            lax.fori_loop(0, count, piece, 0)

        def tile(n, t, kind):
            q = (n - G0) * tiles + t

            if kind == 'first':
                @pl.when(t % 2 == 0)
                def _():
                    item(G0 + 3 + t // 2, 'yf', 'G')
            elif kind == 'middle':
                p = q - tiles

                @pl.when((p == 0) | (4 * p // 19 > 4 * (p - 1) // 19))
                def _():
                    item(G0 + 5 + 4 * p // 19, 'yf', 'W')

            @pl.when(t == 1)
            def _():
                item(n + 1, 'xf', 'G')

            def next_chunk():
                item(n + 1, 'done', 'G')
                for i in range(2):
                    dcopy(wdown, dl, n + 1, i).start()
                if kind == 'middle':
                    @pl.when(n == N - 3)
                    def _():
                        item(N - 1, 'yf', 'G')

            if kind != 'first':
                pl.when((t == tiles - 1) & (n + 1 < N))(next_chunk)

            @pl.when(q + 1 < NG * tiles)
            def _():
                hcopy(q + 1).start()
                if kind == 'last':
                    tail_load(q + 1).start()

            @pl.when(q >= 2)
            def _():
                ycopy(q - 2).wait()
            hcopy(q).wait()
            if kind == 'first':
                ucopy(t).wait()
            if kind == 'last':
                tail_load(q).wait()
                start = (1 - f) * math.prod(OWNK)
                add_dots(q % 2, t, start, start, n % 2, RESTK)
                acc = sb[q % 2]
            else:
                acc = dots(t, n % 2)
            yb[q % 2] = (hb[q % 2].astype(F32) + acc).astype(BF)
            ycopy(q).start()
            if kind == 'first':
                def own(i, _):
                    @pl.when(t > 0)
                    def _():
                        tail_store(t - 1, i).wait()
                    start = math.prod(RESTK)
                    sb[i] = jnp.zeros((MD, FW), F32)
                    add_dots(i, t, f * start, i * HF + f * (start - HF), (G0 + 1) % 2, OWNK)
                    tail_store(t, i).start()
                    return 0
                lax.fori_loop(0, 2, own, 0)
                pl.when(t == tiles - 1)(next_chunk)

        def step(n, kind):
            for i in range(2):
                dcopy(wdown, dl, n, i).wait()
                if kind == 'first':
                    ahead(wdown, dl, i).wait()

            def mt(t, _):
                tile(n, t, kind)
                return 0
            lax.fori_loop(0, tiles, mt, 0)
            return 0

        step(jnp.int32(G0), 'first')
        for i in range(2):
            tail_store(tiles - 1, i).wait()
        tail_load(jnp.int32((NG - 2) * tiles)).start()
        lax.fori_loop(G0 + 1, N - 2, lambda n, _: step(n, 'middle'), 0)
        lax.fori_loop(N - 2, N, lambda n, _: step(n, 'last'), 0)
        for q in (NG * tiles - 2, NG * tiles - 1):
            ycopy(jnp.int32(q)).wait()

    def last_scope(wdown, dl):
        dma = pltpu.SemaphoreType.DMA
        pl.run_scoped(functools.partial(scope, wdown, dl), pltpu.VMEM((2, TOK, HD), BF), pltpu.VMEM((SLOTS, 2, HD, CW), BF), pltpu.VMEM((2, TOK, CW), BF),
                      dma((SLOTS, 4)), dma((2,)))
        pl.run_scoped(functools.partial(down_phase, wdown, dl), pltpu.VMEM((TOK, FFN), BF), pltpu.VMEM((2, MD, FW), BF), pltpu.VMEM((2, MD, FW), BF),
                      pltpu.VMEM((2, MD, FW), F32), dma((TOK // MD,)), dma((2,)), dma((2,)), dma((2,)))

    pl.run_scoped(last_scope, pltpu.VMEM((2, FFN, FW), BF), pltpu.SemaphoreType.DMA((2, 2)))


def local_layer(x_loc, norm_attn, w_query, w_key, w_value, w_out, norm_mlp, w_gate, w_up, w_down):
    shape = x_loc.shape
    x2 = x_loc.reshape(TOK, D)
    anys = pl.BlockSpec(memory_space=pl.ANY)
    vm = pl.BlockSpec(memory_space=pltpu.VMEM)

    def out(*sh):
        return jax.ShapeDtypeStruct(sh, BF)
    sem = pltpu.SemaphoreType.DMA
    res = pl.pallas_call(
        kernel,
        out_shape=[out(TOK, D), out(ROWS * SEQ, D), out(HD, D), out(HD, D), out(HD, D), out(HD, D), out(HD, FFN), out(HD, FFN), out(HF, D),
                   out(TOK, D), out(3, ROWS * LN, HD), jax.ShapeDtypeStruct((TOK, D), F32), out(TOK, FFN), out(TOK, D)],
        in_specs=[anys, vm, vm] + [anys] * 7,
        out_specs=[anys] * 14,
        scratch_shapes=[pltpu.VMEM((2, HD // LN, LN), F32)] * 2 + [pltpu.VMEM((4, 1, HD), F32)]
        + [sem((YR,))] * 2 + [sem((XR,))] * 6 + [sem((2,)), sem((ROWS, 3)), sem((ROWS, 3)), sem((3,)), sem((3,))],
        compiler_params=pltpu.CompilerParams(collective_id=0, has_side_effects=True, vmem_limit_bytes=66_900_000),
        cost_estimate=pl.CostEstimate(flops=846 * 10**9, bytes_accessed=10**9, transcendentals=0),
        name='layer',
    )(x2, norm_attn.reshape(HD // LN, LN), norm_mlp.reshape(HD // LN, LN), w_query, w_key, w_value, w_out, w_gate, w_up, w_down)
    return res[0].reshape(shape)


def solution(mesh):
    rows = P(('dp', 'fsdp'), 'sp', None)
    weight = P('fsdp', None)
    gain = P('fsdp')
    specs = (rows, gain, weight, weight, weight, weight, gain, weight, weight, weight)
    return jax.shard_map(local_layer, mesh=mesh, in_specs=specs, out_specs=rows, check_vma=False)
```

```python
import math
import functools
import jax
import jax.numpy as jnp
from jax import lax
from jax.experimental import pallas as pl
from jax.experimental.pallas import tpu as pltpu
from jax.sharding import PartitionSpec as P

HEAD = 128
LN = HEAD
SEQ = 512
EPS = 1e-5
THETA = 5e7
NEG = -1e30
BF = jnp.bfloat16
F32 = jnp.float32
MESH = pl.DeviceIdType.MESH

D = 4096
HD = D // 2
FFN = 11008
HF = FFN // 2
TOK = 2048
GW = 256
CW = 512
FW = 256
ROWS = 8

NC, NE, NF, NG = 8, 8, 43, 16
E0 = NC
F0 = E0 + NE
G0 = F0 + NF
N = G0 + NG
YR, XR = 64, 32
FD = F0 + 3
F_E = 512
G_E = 1360
G_L = 352
YAHEAD = 16
SLOTS = 2
KB = 1024
KSPLIT = tuple(range(0, FFN - 1792, 1792)) + (FFN,)
OWNK = 3, 1792
RESTK = 2, 2816
MT = 1024
NB = 64
MD = 512


def kernel(x_in, gattn, gmlp, wq, wk, wv, wo, wg, wu, wd,
           y, xr, rq, rk, rv, ro, rg, ru, rd, ob, ostage, psum, ubuf, hbuf,
           gown, grem, gains, ys, yr, xs, xrs, dys, dyr, dxs, dxr, gsem, xsend, xrecv, osend, orecv):
    f = lax.axis_index('fsdp')
    s = lax.axis_index('sp')
    cx = s // 2
    cc = s % 2
    ynbr = (0, 1 - f, s)
    xnbr = (0, f, (s + 2) % 4)
    pnbr = (0, f, cx * 2 + 1 - cc)

    def peer(k):
        if k == 1:
            return cx * 2 + 1 - cc
        if k == 2:
            return (s + 2) % 4
        return 3 - s

    bar = pltpu.get_barrier_semaphore()
    for dev in (ynbr, pnbr, xnbr, (0, f, 3 - s)):
        pl.semaphore_signal(bar, inc=1, device_id=dev, device_id_type=MESH)
    pl.semaphore_wait(bar, 4)

    def rcopy(src, dst, ssem, rsem, dev):
        return pltpu.make_async_remote_copy(src_ref=src, dst_ref=dst, send_sem=ssem, recv_sem=rsem, device_id=dev, device_id_type=MESH)

    class Part:
        def __init__(self, w, r, col, ncol, half, e, sem):
            self.w, self.r, self.half, self.e, self.m = w, r, half, e, half - 2 * e
            self.ysem, self.sem = sem % YR, sem % XR
            self.cols = pl.ds(col, ncol)

        def rows(self, off, n):
            return pl.ds(pl.multiple_of(cc * self.half + off, 16), n)

        def ycopy(self):
            a = (self.rows(cx * self.e, self.e + self.m), self.cols)
            return rcopy(self.w.at[a], self.r.at[a], ys.at[self.ysem], yr.at[self.ysem], ynbr)

        def xcopy(self):
            a = (self.rows(cx * (self.e + self.m), self.e), self.cols)
            return rcopy(self.r.at[a], self.r.at[a], xs.at[self.sem], xrs.at[self.sem], xnbr)

        def dycopy(self):
            a = (self.rows(cx * self.e, self.e + self.m), self.cols)
            return rcopy(self.r.at[a], self.r.at[a], dys.at[self.sem], dyr.at[self.sem], pnbr)

        def dxcopy(self):
            a = (self.rows((1 - cx) * (self.e + self.m), self.e), self.cols)
            return rcopy(self.r.at[a], self.r.at[a], dxs.at[self.sem], dxr.at[self.sem], pnbr)

        def ysend(self):
            self.ycopy().start()

        def yf(self):
            c = self.ycopy()
            c.wait_recv()
            if self.e:
                self.xcopy().start()
            self.dycopy().start()
            c.wait_send()

        def xf(self):
            if self.e:
                c = self.xcopy()
                c.wait_recv()
                self.dxcopy().start()
                c.wait_send()

        def done(self):
            c = self.dycopy()
            c.wait_recv()
            c.wait_send()
            if self.e:
                c = self.dxcopy()
                c.wait_recv()
                c.wait_send()

    def al(v, k):
        return v if isinstance(v, int) else pl.multiple_of(v, k)

    def when(cond, fn):
        if isinstance(cond, bool):
            if cond:
                fn()
        else:
            pl.when(cond)(fn)

    def item(n, what, cand):
        def run(pairs, col, ncol, half, e, sem):
            for i, (w, r) in enumerate(pairs):
                getattr(Part(w, r, col, ncol, half, e, sem + i), what)()

        if 'C' in cand:
            when(n < E0, lambda: run(((wq, rq), (wk, rk), (wv, rv)), pl.multiple_of(cx * HD + n * GW, GW), GW, HD // 2, 0, 3 * n))
        if 'E' in cand:
            when((n >= E0) & (n < F0), lambda: run(((wo, ro),), al((n - E0) * CW, CW), CW, HD // 2, 0, n + 2 * NC))
        if 'F' in cand:
            pairs = ((wg, rg), (wu, ru))
            if 'D' in cand:
                when((n >= F0) & (n < FD), lambda: run(pairs, al((n - F0) * FW, FW), FW, HD // 2, 0, 2 * n + 2 * NC - F0))
            when((n >= FD) & (n < G0), lambda: run(pairs, al((n - F0) * FW, FW), FW, HD // 2, F_E, 2 * n + 2 * NC - F0))
        if 'W' in cand or 'G' in cand:
            when((n >= G0) & (n < N - 1), lambda: run(((wd, rd),), al((n - G0) * FW, FW), FW, HF // 2, G_E, n + 2 * NC + NF))
        if 'G' in cand:
            when(n == N - 1, lambda: run(((wd, rd),), D - FW, FW, HF // 2, G_L, n + 2 * NC + NF))

    gown[0] = gattn[...].astype(F32)
    gown[1] = gmlp[...].astype(F32)
    gcopy = rcopy(gown, grem, gsem.at[0], gsem.at[1], ynbr)
    gcopy.start()
    item(0, 'ysend', 'C')

    def xcopy(r, k):
        first = (cc if k == 2 else 1 - cc) * ROWS
        src = x_in.at[pl.ds(pl.multiple_of((first + r) * LN, LN), LN)]
        dst = xr.at[pl.ds(pl.multiple_of(r * SEQ + s * LN, LN), LN)]
        return rcopy(src, dst, xsend.at[r, k - 1], xrecv.at[r, k - 1], (0, f, peer(k)))

    for r in range(ROWS):
        for k in (2, 3, 1):
            xcopy(r, k).start()
    for n in range(1, 4):
        item(n, 'ysend', 'C')

    def positions(shape, dim):
        j = lax.broadcasted_iota(jnp.int32, shape, dim)
        return (j % LN) * 4 + j // LN

    gcopy.wait_recv()
    gcopy.wait_send()
    for g in range(2):
        for i, src in enumerate((gown, grem)):
            v = src[g]
            gains[2 * g + i] = jnp.concatenate([v[k:k + 1] for k in range(HD // LN)], axis=1)

    def norm_tile(act, xt, t, row, g):
        def sub(i, _):
            for o in range(0, NB, 16):
                rs = pl.ds(pl.multiple_of(i * NB + o, 16), 16)
                x0 = xt[t, 0, rs, :].astype(F32)
                x1 = xt[t, 1, rs, :].astype(F32)
                ss = jnp.sum(x0 * x0, axis=-1, keepdims=True) + jnp.sum(x1 * x1, axis=-1, keepdims=True)
                inv = lax.rsqrt(ss * (1.0 / D) + EPS)
                to = pl.ds(pl.multiple_of(row + i * NB + o, 16), 16)
                act[0, to, :] = (xt[t, 0, rs, :].astype(F32) * inv * gains[2 * g]).astype(BF)
                act[1, to, :] = (xt[t, 1, rs, :].astype(F32) * inv * gains[2 * g + 1]).astype(BF)
            return 0
        lax.fori_loop(0, LN // NB, sub, 0)

    def halves(src, row, xt, t, sem):
        rows = pl.ds(row, LN)
        return [pltpu.make_async_copy(src.at[rows, pl.ds(pl.multiple_of(h * HD, HD), HD)], xt.at[t, i], sem.at[t, i])
                for i, h in enumerate((f, 1 - f))]

    def product(act, rows, wbuf, slot):
        acc = None
        for i in range(2):
            for k in range(0, HD, KB):
                part = jnp.dot(act[i, rows, k:k + KB], wbuf[slot, i, k:k + KB], preferred_element_type=F32)
                acc = part if acc is None else acc + part
        return acc

    def oremote(k):
        first = cc * ROWS * LN
        return rcopy(ostage.at[k - 1], ob.at[pl.ds(pl.multiple_of(first, LN), ROWS * LN), pl.ds(pl.multiple_of(cx * HD, HD), HD)],
                     osend.at[k - 1], orecv.at[k - 1], (0, f, peer(k)))

    def attention_phase(cos, sin, qpos, act, wbuf, obuf, xt, qb, kb, vb, wl, ol, xl):
        def table(i, _):
            rs = pl.ds(pl.multiple_of(i * LN, LN), LN)
            pos = lax.broadcasted_iota(jnp.int32, (LN, HEAD), 0) * 4 + i
            lane = lax.broadcasted_iota(jnp.int32, (LN, HEAD), 1)
            freq = jnp.exp((lane % (HEAD // 2)).astype(F32) * (-2.0 * math.log(THETA) / HEAD))
            ang = pos.astype(F32) * freq
            qpos[rs, :] = pos
            cos[rs, :] = jnp.cos(ang)
            sn = jnp.sin(ang)
            sin[rs, :] = jnp.where(lane < HEAD // 2, -sn, sn)
            return 0
        lax.fori_loop(0, 4, table, 0)

        def wcopies(j, slot):
            cols = pl.ds(pl.multiple_of(cx * HD + j * GW, GW), GW)
            return [pltpu.make_async_copy(b.at[:, cols], wbuf.at[slot, i, :, pl.ds(t * GW, GW)], wl.at[slot, i, t])
                    for t, pair in enumerate(((wq, rq), (wk, rk), (wv, rv))) for i, b in enumerate(pair)]

        def tokens(r):
            for k in (1, 2, 3):
                c = xcopy(r, k)
                c.wait_recv()
                c.wait_send()

            def cps(t):
                return halves(xr, pl.multiple_of(r * SEQ + t * LN, LN), xt, t, xl)
            for t in range(4):
                @pl.when(s != t)
                def _():
                    for c in cps(t):
                        c.start()

                @pl.when(s == t)
                def _():
                    for c in halves(x_in, pl.multiple_of((cc * ROWS + r) * LN, LN), xt, t, xl):
                        c.start()
            for t in range(4):
                for c in cps(t):
                    c.wait()
                norm_tile(act, xt, t, r * SEQ + t * LN, 0)

        def rope(u):
            out = []
            for h in range(GW // HEAD):
                v = u[:, h * HEAD:(h + 1) * HEAD]
                out.append(v * cos[...] + pltpu.roll(v, HEAD // 2, 1) * sin[...])
            return jnp.concatenate(out, axis=1).astype(BF)

        def place(r, j):
            return (pl.ds(pl.multiple_of((cc * ROWS + r) * LN, LN), LN), pl.ds(pl.multiple_of(cx * HD + j * GW, GW), GW))

        def stage(r, j, k):
            return ostage.at[k - 1, pl.ds(pl.multiple_of(r * LN, LN), LN), pl.ds(pl.multiple_of(j * GW, GW), GW)]

        def ostore(r, j, slot):
            own = pltpu.make_async_copy(obuf.at[slot, pl.ds(pl.multiple_of(s * LN, LN), LN)], ob.at[place(r, j)], ol.at[slot, 0])
            return [own] + [pltpu.make_async_copy(obuf.at[slot, pl.ds(pl.multiple_of(peer(k) * LN, LN), LN)], stage(r, j, k), ol.at[slot, k])
                            for k in (1, 2, 3)]

        def osends(r, j, slot):
            for c in ostore(r, j, slot):
                c.wait()
            for k in (2, 3, 1):
                rcopy(stage(r, j, k), ob.at[place(r, j)], osend.at[k - 1], orecv.at[k - 1], (0, f, peer(k))).start()

        def shell(k, _):
            def unit(i, _):
                r = jnp.minimum(i, k)
                j = jnp.minimum(k, 2 * k - i)
                u = k * k + i
                slot = (k * (k + 1) // 2 + k - j) % 2

                def next_group():
                    item(k + 1, 'done', 'C')
                    for c in wcopies(k + 1, 1 - slot):
                        c.start()

                @pl.when(i == k)
                def _():
                    tokens(k)

                    @pl.when((k > 0) & (k < NC - 1))
                    def _():
                        item(k + 1, 'yf', 'C')

                @pl.when((i == 0) | (i > k))
                def _():
                    for c in wcopies(j, slot):
                        c.wait()

                    @pl.when(j > 0)
                    def _():
                        for c in wcopies(j - 1, 1 - slot):
                            c.start()

                    @pl.when((j == 0) & (k > 0) & (k < NC - 1))
                    def _():
                        next_group()

                rows = pl.ds(pl.multiple_of(r * SEQ, SEQ), SEQ)
                acc = product(act, rows, wbuf, slot)
                qb[...] = rope(acc[:, :GW])
                kb[...] = rope(acc[:, GW:2 * GW])
                vb[...] = acc[:, 2 * GW:].astype(BF)

                def head(h, _):
                    hs = pl.ds(pl.multiple_of(h * HEAD, HEAD), HEAD)
                    sc = lax.dot_general(qb[:, hs], kb[:, hs], (((1,), (1,)), ((), ())), preferred_element_type=F32)
                    qp = qpos[...]
                    kp = positions((1, SEQ), 1)
                    sc = jnp.where(jnp.concatenate([qp] * 4, axis=1) >= kp, sc, NEG)
                    mx = jnp.max(sc, axis=-1, keepdims=True)
                    p = jnp.exp2((sc - mx) * (HEAD ** -0.5 * math.log2(math.e)))
                    tot = jnp.sum(p, axis=-1, keepdims=True)
                    o = jnp.dot(p.astype(BF), vb[:, hs], preferred_element_type=F32) / tot
                    obuf[u % 2, :, hs] = o.astype(BF)
                    return 0
                lax.fori_loop(0, GW // HEAD, head, 0)
                for c in ostore(r, j, u % 2):
                    c.start()

                @pl.when(i > 0)
                def _():
                    osends(jnp.minimum(i - 1, k), jnp.minimum(k, 2 * k - i + 1), (u + 1) % 2)

                @pl.when((i == 0) & (k > 0))
                def _():
                    osends(k - 1, 0, (u + 1) % 2)

                @pl.when(u % 4 == 0)
                def _():
                    item(u // 4 + 4, 'ysend', 'CEFD')

                @pl.when(k == 0)
                def _():
                    item(1, 'yf', 'C')
                    next_group()
                return 0
            lax.fori_loop(0, 2 * k + 1, unit, 0)
            return 0

        item(0, 'yf', 'C')
        item(0, 'done', 'C')
        for c in wcopies(jnp.int32(0), jnp.int32(0)):
            c.start()
        lax.fori_loop(0, NC, shell, 0)
        osends(jnp.int32(ROWS - 1), jnp.int32(0), jnp.int32((NC * NC - 1) % 2))

    pl.run_scoped(attention_phase, pltpu.VMEM((SEQ, HEAD), F32), pltpu.VMEM((SEQ, HEAD), F32), pltpu.VMEM((SEQ, LN), jnp.int32), pltpu.VMEM((2, ROWS * SEQ, HD), BF), pltpu.VMEM((2, 2, HD, 3 * GW), BF), pltpu.VMEM((2, SEQ, GW), BF),
                  pltpu.VMEM((4, 2, LN, HD), BF), pltpu.VMEM((SEQ, GW), BF), pltpu.VMEM((SEQ, GW), BF), pltpu.VMEM((SEQ, GW), BF),
                  pltpu.SemaphoreType.DMA((2, 2, 3)), pltpu.SemaphoreType.DMA((2, 4)), pltpu.SemaphoreType.DMA((4, 2)))

    for n in range(E0, F0):
        item(n, 'yf', 'E')
    for n in range(20, 24):
        item(n, 'ysend', 'FD')

    def dcopy(wdown, dl, n, i):
        cols = pl.ds(pl.multiple_of((n - G0) * FW, FW), FW)
        h = (f, 1 - f)[i]
        return pltpu.make_async_copy((wd, rd)[i].at[:, cols], wdown.at[n % 2, pl.ds(pl.multiple_of(h * HF, LN), HF)], dl.at[n % 2, i])

    def ahead(wdown, dl, i):
        slot = (G0 + 1) % 2
        return pltpu.make_async_copy(wd.at[:, pl.ds(D - (2 - i) * FW, FW)], wdown.at[slot, pl.ds(i * HF, HF)], dl.at[slot, i])

    def scope(wdown, dl, act, wbuf, obuf, wl, ol):
        def wcopies(n, cand):
            def go(fn):
                slot = n % SLOTS
                if 'F' in cand:
                    def ff():
                        cols = pl.ds(al((n - F0) * FW, FW), FW)
                        for i, pair in enumerate(((wg, wu), (rg, ru))):
                            for j, b in enumerate(pair):
                                fn(pltpu.make_async_copy(b.at[:, cols], wbuf.at[slot, i, :, pl.ds(j * FW, FW)], wl.at[slot, i + 2 * j]))
                    when((n >= F0) & (n < G0), ff)
            return go

        def load(n, cand):
            wcopies(n, cand)(lambda c: c.start())

        def loaded(n, cand):
            wcopies(n, cand)(lambda c: c.wait())

        def out_phase(hx, pb, hl, pp, al_):
            def ecopy(n, i):
                h = cx if i == 0 else 1 - cx
                cols = pl.ds(al((n - E0) * CW, CW), CW)
                return h, lambda w: pltpu.make_async_copy(w.at[:, cols], wbuf.at[n % SLOTS, i], wl.at[n % SLOTS, i])

            def eload(n, i):
                h, copy = ecopy(n, i)
                pl.when(h == f)(lambda: copy(wo).start())
                pl.when(h != f)(lambda: copy(ro).start())

            def eloaded(n, i):
                ecopy(n, i)[1](wo).wait()

            def acopy(t, i):
                h = cx if i == 0 else 1 - cx
                rows = pl.ds(t * MT, MT)
                return pltpu.make_async_copy(ob.at[rows, pl.ds(pl.multiple_of(h * HD, HD), HD)], act.at[i, rows], al_.at[t, i])

            def cols(n):
                return pl.ds(pl.multiple_of((n - E0) * CW, CW), CW)

            def xload(n):
                return pltpu.make_async_copy(x_in.at[:, cols(n)], hx.at[n % 2], hl.at[n % 2])

            def pstore(n):
                return pltpu.make_async_copy(pb.at[n % 2], psum.at[:, cols(n)], pp.at[0, n % 2])

            def pload(n):
                return pltpu.make_async_copy(psum.at[:, cols(n)], pb.at[n % 2], pp.at[1, n % 2])

            def hstore(n):
                return pltpu.make_async_copy(obuf.at[n % 2], hbuf.at[:, cols(n)], ol.at[n % 2])

            def eproduct(rows, slot, i):
                acc = None
                for k in range(0, HD, KB):
                    part = jnp.dot(act[i, rows, k:k + KB], wbuf[slot, i, k:k + KB], preferred_element_type=F32)
                    acc = part if acc is None else acc + part
                return acc

            first = jnp.int32(E0)
            item(E0, 'done', 'E')
            eload(first, 0)
            xload(first).start()
            c = oremote(1)
            c.wait_recv()
            c.wait_send()
            for t in range(TOK // MT):
                acopy(t, 0).start()
            for t in range(TOK // MT):
                acopy(t, 0).wait()

            def step1(n, _):
                @pl.when(n + 1 < F0)
                def _():
                    item(n + 1, 'done', 'E')
                    eload(n + 1, 0)
                    xload(n + 1).start()

                @pl.when(n >= E0 + 2)
                def _():
                    pstore(n - 2).wait()
                eloaded(n, 0)
                xload(n).wait()

                def mt(t, _):
                    rows = pl.ds(pl.multiple_of(t * MT, MT), MT)
                    pb[n % 2, rows, :] = hx[n % 2, rows, :].astype(F32) + eproduct(rows, n % SLOTS, 0)
                    return 0
                lax.fori_loop(0, TOK // MT, mt, 0)
                pstore(n).start()
                return 0
            lax.fori_loop(E0, F0, step1, 0)
            for n in (F0 - 2, F0 - 1):
                pstore(jnp.int32(n)).wait()
            eload(first, 1)
            pload(first).start()

            for n in range(F0, FD + 1):
                item(n, 'yf', 'FD')
            for k in (2, 3):
                c = oremote(k)
                c.wait_recv()
                c.wait_send()
            for t in range(TOK // MT):
                acopy(t, 1).start()
            for t in range(TOK // MT):
                acopy(t, 1).wait()

            def step2(n, _):
                item(n + YAHEAD, 'ysend', 'F')

                @pl.when((n == E0) | ((n - E0) * 2 // 5 > (n - E0 - 1) * 2 // 5))
                def _():
                    item(FD + 1 + (n - E0) * 2 // 5, 'yf', 'F')

                @pl.when(n + 1 < F0)
                def _():
                    eload(n + 1, 1)
                    pload(n + 1).start()

                @pl.when(n + 1 == F0)
                def _():
                    item(n + 1, 'done', 'FD')
                    load(n + 1, 'F')

                @pl.when(n >= E0 + 2)
                def _():
                    hstore(n - 2).wait()
                eloaded(n, 1)
                pload(n).wait()

                def mt(t, _):
                    rows = pl.ds(pl.multiple_of(t * MT, MT), MT)
                    obuf[n % 2, rows, :] = (pb[n % 2, rows, :] + eproduct(rows, n % SLOTS, 1)).astype(BF)
                    return 0
                lax.fori_loop(0, TOK // MT, mt, 0)
                hstore(n).start()
                return 0
            lax.fori_loop(E0, F0, step2, 0)
            for n in (F0 - 2, F0 - 1):
                hstore(jnp.int32(n)).wait()

        pl.run_scoped(out_phase, pltpu.VMEM((2, TOK, CW), BF), pltpu.VMEM((2, TOK, CW), F32), pltpu.SemaphoreType.DMA((2,)), pltpu.SemaphoreType.DMA((2, 2)),
                      pltpu.SemaphoreType.DMA((2, 2)))

        def norm_phase(xt, xl):
            def cps(i):
                return halves(hbuf, pl.multiple_of(i * LN, LN), xt, i % 4, xl)
            for i in range(3):
                for c in cps(jnp.int32(i)):
                    c.start()
            item(FD + 4, 'yf', 'F')

            def step(i, _):
                @pl.when(i + 3 < 16)
                def _():
                    for c in cps(i + 3):
                        c.start()
                for c in cps(i):
                    c.wait()
                norm_tile(act, xt, i % 4, i * LN, 1)
                return 0
            lax.fori_loop(0, 16, step, 0)

        pl.run_scoped(norm_phase, pltpu.VMEM((4, 2, LN, HD), BF), pltpu.SemaphoreType.DMA((4, 2)))

        def ustore(n):
            return pltpu.make_async_copy(obuf.at[n % 2, :, pl.ds(0, FW)], ubuf.at[:, pl.ds(pl.multiple_of((n - F0) * FW, FW), FW)], ol.at[n % 2])

        def gate_step(n, _):
            @pl.when(n >= F0 + 2)
            def _():
                ustore(n - 2).wait()
            loaded(n, 'F')
            slot = n % SLOTS

            def mt(t, _):
                @pl.when(t == 0)
                def _():
                    item(n + YAHEAD, 'ysend', 'FG')

                    @pl.when((n == F0) | ((n - F0) * 8 // 9 > (n - F0 - 1) * 8 // 9))
                    def _():
                        item(FD + 5 + (n - F0) * 8 // 9, 'yf', 'FG')
                    item(n + 1, 'xf', 'FG')

                @pl.when(t == 1)
                def _():
                    item(n + 1, 'done', 'FGD')
                    load(n + 1, 'F')

                    @pl.when(n + 1 == G0)
                    def _():
                        for i in range(2):
                            dcopy(wdown, dl, n + 1, i).start()
                            ahead(wdown, dl, i).start()
                rows = pl.ds(pl.multiple_of(t * MT, MT), MT)
                acc = product(act, rows, wbuf, slot)
                gate, up = acc[:, :FW], acc[:, FW:]
                obuf[n % 2, rows, pl.ds(0, FW)] = (gate * jax.nn.sigmoid(gate) * up).astype(BF)
                return 0
            lax.fori_loop(0, TOK // MT, mt, 0)
            ustore(n).start()
            return 0
        lax.fori_loop(F0, G0, gate_step, 0)
        for n in (G0 - 2, G0 - 1):
            ustore(jnp.int32(n)).wait()

    def down_phase(wdown, dl, u, hb, yb, sb, ul, hl, yl, sl):
        tiles = TOK // MD

        def ucopy(t):
            rows = pl.ds(pl.multiple_of(t * MD, MD), MD)
            return pltpu.make_async_copy(ubuf.at[rows], u.at[rows], ul.at[t])

        def at(q):
            return pl.ds(pl.multiple_of((q % tiles) * MD, MD), MD), pl.ds(pl.multiple_of((q // tiles) * FW, FW), FW)

        def hcopy(q):
            return pltpu.make_async_copy(hbuf.at[at(q)], hb.at[q % 2], hl.at[q % 2])

        def ycopy(q):
            return pltpu.make_async_copy(yb.at[q % 2], y.at[at(q)], yl.at[q % 2])

        hcopy(jnp.int32(0)).start()
        for t in range(tiles):
            ucopy(t).start()

        def tail_copy(t, i):
            rows = pl.ds(pl.multiple_of(t * MD, MD), MD)
            return psum.at[rows, pl.ds(pl.multiple_of(D + (i - 2) * FW, FW), FW)]

        def tail_store(t, i):
            return pltpu.make_async_copy(sb.at[i], tail_copy(t, i), sl.at[i])

        def tail_load(q):
            return pltpu.make_async_copy(tail_copy(q % tiles, q // tiles - (NG - 2)), sb.at[q % 2], sl.at[q % 2])

        def dots(t, slot):
            rows = pl.ds(pl.multiple_of(t * MD, MD), MD)
            acc = None
            for a, b in zip(KSPLIT, KSPLIT[1:]):
                part = jnp.dot(u[rows, a:b], wdown[slot, a:b], preferred_element_type=F32)
                acc = part if acc is None else acc + part
            return acc

        def add_dots(i, t, ustart, wstart, slot, pieces):
            count, k = pieces
            rows = pl.ds(pl.multiple_of(t * MD, MD), MD)

            def piece(j, _):
                us = pl.ds(pl.multiple_of(ustart + j * k, 2 * LN), k)
                ws = pl.ds(pl.multiple_of(wstart + j * k, LN), k)
                sb[i] += jnp.dot(u[rows, us], wdown[slot, ws], preferred_element_type=F32)
                return 0
            lax.fori_loop(0, count, piece, 0)

        def tile(n, t, kind):
            q = (n - G0) * tiles + t

            if kind == 'first':
                @pl.when(t % 2 == 0)
                def _():
                    item(G0 + 3 + t // 2, 'yf', 'G')
            elif kind == 'middle':
                p = q - tiles

                @pl.when((p == 0) | (4 * p // 19 > 4 * (p - 1) // 19))
                def _():
                    item(G0 + 5 + 4 * p // 19, 'yf', 'W')

            @pl.when(t == 1)
            def _():
                item(n + 1, 'xf', 'G')

            def next_chunk():
                item(n + 1, 'done', 'G')
                for i in range(2):
                    dcopy(wdown, dl, n + 1, i).start()
                if kind == 'middle':
                    @pl.when(n == N - 3)
                    def _():
                        item(N - 1, 'yf', 'G')

            if kind != 'first':
                pl.when((t == tiles - 1) & (n + 1 < N))(next_chunk)

            @pl.when(q + 1 < NG * tiles)
            def _():
                hcopy(q + 1).start()
                if kind == 'last':
                    tail_load(q + 1).start()

            @pl.when(q >= 2)
            def _():
                ycopy(q - 2).wait()
            hcopy(q).wait()
            if kind == 'first':
                ucopy(t).wait()
            if kind == 'last':
                tail_load(q).wait()
                start = (1 - f) * math.prod(OWNK)
                add_dots(q % 2, t, start, start, n % 2, RESTK)
                acc = sb[q % 2]
            else:
                acc = dots(t, n % 2)
            yb[q % 2] = (hb[q % 2].astype(F32) + acc).astype(BF)
            ycopy(q).start()
            if kind == 'first':
                def own(i, _):
                    @pl.when(t > 0)
                    def _():
                        tail_store(t - 1, i).wait()
                    start = math.prod(RESTK)
                    sb[i] = jnp.zeros((MD, FW), F32)
                    add_dots(i, t, f * start, i * HF + f * (start - HF), (G0 + 1) % 2, OWNK)
                    tail_store(t, i).start()
                    return 0
                lax.fori_loop(0, 2, own, 0)
                pl.when(t == tiles - 1)(next_chunk)

        def step(n, kind):
            for i in range(2):
                dcopy(wdown, dl, n, i).wait()
                if kind == 'first':
                    ahead(wdown, dl, i).wait()

            def mt(t, _):
                tile(n, t, kind)
                return 0
            lax.fori_loop(0, tiles, mt, 0)
            return 0

        step(jnp.int32(G0), 'first')
        for i in range(2):
            tail_store(tiles - 1, i).wait()
        tail_load(jnp.int32((NG - 2) * tiles)).start()
        lax.fori_loop(G0 + 1, N - 2, lambda n, _: step(n, 'middle'), 0)
        lax.fori_loop(N - 2, N, lambda n, _: step(n, 'last'), 0)
        for q in (NG * tiles - 2, NG * tiles - 1):
            ycopy(jnp.int32(q)).wait()

    def last_scope(wdown, dl):
        dma = pltpu.SemaphoreType.DMA
        pl.run_scoped(functools.partial(scope, wdown, dl), pltpu.VMEM((2, TOK, HD), BF), pltpu.VMEM((SLOTS, 2, HD, CW), BF), pltpu.VMEM((2, TOK, CW), BF),
                      dma((SLOTS, 4)), dma((2,)))
        pl.run_scoped(functools.partial(down_phase, wdown, dl), pltpu.VMEM((TOK, FFN), BF), pltpu.VMEM((2, MD, FW), BF), pltpu.VMEM((2, MD, FW), BF),
                      pltpu.VMEM((2, MD, FW), F32), dma((TOK // MD,)), dma((2,)), dma((2,)), dma((2,)))

    pl.run_scoped(last_scope, pltpu.VMEM((2, FFN, FW), BF), pltpu.SemaphoreType.DMA((2, 2)))


def hand_over(src, dst, buf, isem, osem):
    count, rows, _ = buf.shape
    parts = [pl.ds(i * rows, rows) for i in range(count)]
    loads = [pltpu.make_async_copy(src.at[p], buf.at[i], isem.at[i]) for i, p in enumerate(parts)]
    stores = [pltpu.make_async_copy(buf.at[i], dst.at[p], osem.at[i]) for i, p in enumerate(parts)]
    for c in loads:
        c.start()
    for a, b in zip(loads, stores):
        a.wait()
        b.start()
    for c in stores:
        c.wait()


def local_layer(x_loc, norm_attn, w_query, w_key, w_value, w_out, norm_mlp, w_gate, w_up, w_down):
    shape = x_loc.shape
    x2 = x_loc.reshape(TOK, D)
    anys = pl.BlockSpec(memory_space=pl.ANY)
    vm = pl.BlockSpec(memory_space=pltpu.VMEM)

    def out(*sh):
        return jax.ShapeDtypeStruct(sh, BF)
    sem = pltpu.SemaphoreType.DMA
    res = pl.pallas_call(
        kernel,
        out_shape=[out(TOK, D), out(ROWS * SEQ, D), out(HD, D), out(HD, D), out(HD, D), out(HD, D), out(HD, FFN), out(HD, FFN), out(HF, D),
                   out(TOK, D), out(3, ROWS * LN, HD), jax.ShapeDtypeStruct((TOK, D), F32), out(TOK, FFN), out(TOK, D)],
        in_specs=[anys, vm, vm] + [anys] * 7,
        out_specs=[anys] * 14,
        scratch_shapes=[pltpu.VMEM((2, HD // LN, LN), F32)] * 2 + [pltpu.VMEM((4, 1, HD), F32)]
        + [sem((YR,))] * 2 + [sem((XR,))] * 6 + [sem((2,)), sem((ROWS, 3)), sem((ROWS, 3)), sem((3,)), sem((3,))],
        compiler_params=pltpu.CompilerParams(collective_id=0, has_side_effects=True, vmem_limit_bytes=66_900_000),
        cost_estimate=pl.CostEstimate(flops=846 * 10**9, bytes_accessed=10**9, transcendentals=0),
        name='layer',
    )(x2, norm_attn.reshape(HD // LN, LN), norm_mlp.reshape(HD // LN, LN), w_query, w_key, w_value, w_out, w_gate, w_up, w_down)
    count = 16
    y = pl.pallas_call(
        hand_over,
        out_shape=out(TOK, D),
        in_specs=[anys],
        out_specs=anys,
        scratch_shapes=[pltpu.VMEM((count, TOK // count, D), BF), sem((count,)), sem((count,))],
        cost_estimate=pl.CostEstimate(flops=0, bytes_accessed=4 * TOK * D, transcendentals=0),
        name='hand_over',
    )(res[0])
    return y.reshape(shape)


def solution(mesh):
    rows = P(('dp', 'fsdp'), 'sp', None)
    weight = P('fsdp', None)
    gain = P('fsdp')
    specs = (rows, gain, weight, weight, weight, weight, gain, weight, weight, weight)
    return jax.shard_map(local_layer, mesh=mesh, in_specs=specs, out_specs=rows, check_vma=False)
```
